32 devices in a mesh: row: 8 (over z, core), col: 4 (over y, x).
Axes of the slice: x: 2, y: 2, z: 4, core: 2. Of those that a mesh axis runs over, the one named last changes fastest.
Arguments:
- ancestor_inverse: float32 [12288, 12288], P('row', 'col'), may hold values from -6 to 6
- panel: float32 [5632, 512], P('col', 'row'), may hold values from -0.078125 to 0.078125
- unit_inverse: float32 [512, 512], P('row'), may hold values from -1 to 1, as said below
- pivot_inverse: float32 [512, 512], P('row', 'col'), may hold values from -6 to 6
- panel_blocks: int32 [44], replicated, may hold values from 0 to 95, as said below
Outputs:
- inverse_row: float32 [512, 12288], P('col', 'row')
- diagonal_block: float32 [512, 512], P('row', 'col')
The draws below stay inside these ranges and needn't reach their ends.
Inputs may be any that keep to these rules, and one draw needn't show every extreme that they name: `panel_blocks`: Distinct, in no particular order. Among the window blocks c * 24 to c * 24 + 23 of any process column c at most 12 are listed, and exactly 12 for some columns. `unit_inverse`: unit lower triangular: ones on the diagonal, zeros above it.
All inputs are finite; a program needn't handle non-finite values.
Results may differ from the reference program's by a relative error of at most 0.00011.
Values sent between devices are 32-bit elements; how exact they have to be, the bound alone decides.
A program may use at most 128 MiB of HBM per device.

```python
import jax
import jax.numpy as jnp
from jax import lax

W = 512
BLK = 128
NWB = 96
R = 12288
PB = 44
P_SIZE = 5632
N_COL = 4


def draw_panel_blocks(key, part):
    range_blocks = NWB // N_COL
    slot_count = range_blocks // 2
    column_order = jax.random.permutation(jax.random.fold_in(key, 11), N_COL)
    counts_used = jnp.where(column_order % 2 == 0, slot_count, slot_count - 2)
    base_ranks = jnp.tile(jnp.arange(range_blocks, dtype=jnp.int32)[None, :], (N_COL, 1))
    ranks = jax.random.permutation(jax.random.fold_in(key, 12), base_ranks, axis=1, independent=True)
    chosen = ranks < counts_used[:, None]
    first_local = jnp.argmax(chosen.astype(jnp.int32), axis=1).astype(jnp.int32)
    firsts = jnp.arange(N_COL, dtype=jnp.int32) * range_blocks + first_local
    local_ids = jnp.arange(range_blocks, dtype=jnp.int32)[None, :]
    rest_mask = (chosen & (local_ids != first_local[:, None])).reshape(-1).astype(jnp.int32)
    per_shard = PB // N_COL
    rest_ids = jnp.argsort(1 - rest_mask, stable=True)[:PB - N_COL].astype(jnp.int32)
    rest_part = rest_ids.reshape(N_COL, per_shard - 1)
    leading = jnp.roll(firsts, -(N_COL // 2))
    stored = jnp.concatenate([leading[:, None], rest_part], axis=1).reshape(-1)
    return stored.astype(jnp.int32)


def draw_unit_inverse(key, part):
    spread = 0.5 / W ** 0.5
    entries = jax.random.truncated_normal(jax.random.fold_in(key, 21), -4.0, 4.0, (W, W), jnp.float32) * spread
    row_ids = jnp.arange(W, dtype=jnp.int32)[:, None]
    col_ids = jnp.arange(W, dtype=jnp.int32)[None, :]
    below = jnp.where(row_ids > col_ids, entries, 0.0)
    return (below + jnp.where(row_ids == col_ids, 1.0, 0.0)).astype(jnp.float32)


def block_scale(stream_key, extent, shards, low, high):
    factor_of, own = 1.0, jax.random.fold_in(stream_key, 6)
    for axis_at, shards_of in shards:
        steps = jnp.exp(jax.random.uniform(jax.random.fold_in(own, axis_at), (shards_of,), jnp.float32, low / len(shards), high / len(shards)))
        factor_of = factor_of * jnp.repeat(steps, extent[axis_at] // shards_of).reshape([-1 if axis == axis_at else 1 for axis in range(len(extent))])
    return factor_of


def bell_draw(rng, dims, width, bound, split=(), kind=jnp.bfloat16):
    drawn = width * jax.random.normal(rng, dims, jnp.float32)
    if split:
        drawn = drawn * block_scale(rng, dims, split, -0.22, 0.18)
    return jnp.clip(drawn, -bound, bound).astype(kind)


def setup_inputs(seed: int = 0) -> dict:
    streams_of = jax.random.split(jax.random.key(seed), 6)
    return {
        "ancestor_inverse": bell_draw(streams_of[0], (R, R), 1.0, 6.0, ((0, 8), (1, 4)), jnp.float32),
        "panel": bell_draw(streams_of[1], (P_SIZE, W), P_SIZE ** -0.5, 0.078125, ((0, 4), (1, 8)), jnp.float32),
        "unit_inverse": draw_unit_inverse(jax.random.fold_in(streams_of[5], 71), 0),
        "pivot_inverse": bell_draw(streams_of[3], (W, W), 1.0, 6.0, ((0, 8), (1, 4)), jnp.float32),
        "panel_blocks": draw_panel_blocks(jax.random.fold_in(streams_of[5], 71), 0),
    }


def reference(ancestor_inverse, panel, unit_inverse, pivot_inverse, panel_blocks):
    highest = lax.Precision.HIGHEST
    normal = jnp.dot(panel, unit_inverse, precision=highest, preferred_element_type=jnp.float32)
    blocked = ancestor_inverse.reshape(R, NWB, BLK)
    columns = jnp.take(blocked, panel_blocks, axis=1).reshape(R, PB * BLK)
    column_inverse = -jnp.dot(columns, normal, precision=highest, preferred_element_type=jnp.float32)
    listed = jnp.take(column_inverse.reshape(NWB, BLK, W), panel_blocks, axis=0).reshape(PB * BLK, W)
    product = jnp.dot(normal.T, listed, precision=highest, preferred_element_type=jnp.float32)
    diagonal_block = pivot_inverse - product
    return column_inverse.T, diagonal_block
```

```python
import functools

import jax
import jax.numpy as jnp
from jax import lax
from jax.experimental import pallas as pl
from jax.experimental.pallas import tpu as pltpu
from jax.sharding import PartitionSpec as P

BLK = 128
NT = (((1,), (1,)), ((), ()))
NN = (((1,), (0,)), ((), ()))
MESH = pl.DeviceIdType.MESH


def select_kernel(per_shard, ids_ref, live_ref, gathered_ref, out_ref):
    slots = out_ref.shape[2] // BLK
    for target in range(out_ref.shape[0]):
        for slot in range(slots):
            at = target * slots + slot
            block = ids_ref[at]
            start = pl.multiple_of((block % per_shard) * BLK, BLK)
            value = gathered_ref[block // per_shard, :, pl.ds(start, BLK)]
            out_ref[target, :, slot * BLK : (slot + 1) * BLK] = jnp.where(
                live_ref[at] > 0, value, 0.0
            )


def select(gathered, ids, live, targets):
    slots = ids.shape[0] // targets
    per_shard = gathered.shape[2] // BLK
    smem = pl.BlockSpec(memory_space=pltpu.SMEM)
    vmem = pl.BlockSpec(memory_space=pltpu.VMEM)
    return pl.pallas_call(
        functools.partial(select_kernel, per_shard),
        out_shape=jax.ShapeDtypeStruct((targets, gathered.shape[1], slots * BLK), jnp.float32),
        in_specs=[smem, smem, vmem],
        out_specs=vmem,
    )(ids, live, gathered)


def halves(value):
    high = value.astype(jnp.bfloat16)
    return high, (value - high.astype(jnp.float32)).astype(jnp.bfloat16)


def product_kernel(group, ids_ref, normal_ref, *refs):
    out_ref = refs[group]

    @pl.when(pl.program_id(1) == 0)
    def _():
        out_ref[...] = jnp.zeros_like(out_ref)

    n_high, n_low = halves(normal_ref[...])
    if group == 1:
        block = refs[0][...]
    else:
        block = jnp.concatenate([ref[...] for ref in refs[:group]], axis=1)
    a_high, a_low = halves(block)
    dot = functools.partial(
        lax.dot_general, dimension_numbers=NT, preferred_element_type=jnp.float32
    )
    out_ref[...] -= dot(n_high, a_high) + (dot(n_high, a_low) + dot(n_low, a_high))


def product(normal, ancestor, ids):
    width, slots = normal.shape[0], ids.shape[0]
    rows = ancestor.shape[0]
    group = 2 if slots % 2 == 0 else 1
    tile = 512 if rows % 512 == 0 else BLK

    def column(k):
        return pl.BlockSpec((tile, BLK), lambda i, j, ids: (i, ids[j * group + k]))

    return pl.pallas_call(
        functools.partial(product_kernel, group),
        out_shape=jax.ShapeDtypeStruct((width, rows), jnp.float32),
        grid_spec=pltpu.PrefetchScalarGridSpec(
            num_scalar_prefetch=1,
            grid=(rows // tile, slots // group),
            in_specs=[pl.BlockSpec((width, group * BLK), lambda i, j, ids: (0, j))]
            + [column(k) for k in range(group)],
            out_specs=pl.BlockSpec((width, tile), lambda i, j, ids: (0, i)),
        ),
        compiler_params=pltpu.CompilerParams(
            dimension_semantics=("arbitrary", "arbitrary"), vmem_limit_bytes=32 << 20
        ),
        cost_estimate=pl.CostEstimate(
            flops=6 * width * rows * slots * BLK,
            bytes_accessed=4 * (rows * slots * BLK + 2 * width * rows),
            transcendentals=0,
        ),
    )(ids, normal, *([ancestor] * group))


def on_device(ancestor_inverse, panel, unit_inverse, pivot_inverse, panel_blocks):
    high = lax.Precision.HIGH
    col_index = lax.axis_index("col")
    rows_here, cols_here = ancestor_inverse.shape
    width = unit_inverse.shape[1]
    block_total = panel_blocks.shape[0]
    range_blocks = cols_here // BLK
    row_blocks = rows_here // BLK
    first_block = col_index * range_blocks
    slot_count = range_blocks // 2

    gathered = lax.all_gather(panel.T, "col", axis=0, tiled=False)
    half = width // 2
    unit = [
        lax.all_gather(unit_inverse[:, k * half : (k + 1) * half], "row", axis=0, tiled=True)
        for k in range(2)
    ]

    in_range = (panel_blocks >= first_block) & (panel_blocks < first_block + range_blocks)
    order = jnp.arange(block_total, dtype=jnp.int32)
    upto = order[None, :] <= order[:, None]
    rank_of = jnp.sum((upto & in_range[None, :]).astype(jnp.int32), axis=1) - 1
    slot_ids = jnp.arange(slot_count, dtype=jnp.int32)
    selected = in_range[None, :] & (rank_of[None, :] == slot_ids[:, None])
    stored_ids = jnp.sum(jnp.where(selected, order[None, :], 0), axis=1)
    chosen_ids = jnp.sum(jnp.where(selected, panel_blocks[None, :], 0), axis=1)
    slot_live = jnp.sum(selected.astype(jnp.int32), axis=1)
    local_ids = jnp.clip(chosen_ids - first_block, 0, range_blocks - 1)
    gathered, unit = lax.optimization_barrier((gathered, unit))
    unit = jnp.concatenate(unit, axis=1)
    rows, cols = lax.axis_size("row"), lax.axis_size("col")
    chosen = select(gathered, stored_ids, slot_live, 1)[0]
    window = lax.all_gather(chosen, "row", axis=0, tiled=True)

    match = panel_blocks[None, :] == jnp.arange(rows * row_blocks, dtype=jnp.int32)[:, None]
    block_ids = jnp.sum(jnp.where(match, order[None, :], 0), axis=1)
    block_live = jnp.sum(match.astype(jnp.int32), axis=1)
    part = panel.shape[1] // cols
    share = lax.dynamic_slice_in_dim(gathered, col_index * part, part, 1)
    listed = lax.all_to_all(select(share, block_ids, block_live, rows), "row", 0, 0)
    listed = lax.all_gather(listed, "col", axis=0, tiled=False).reshape(width, rows_here)
    unit_mixed = unit.reshape(rows, cols, part, width).transpose(1, 0, 2, 3).reshape(width, width)

    def normalise(factor, value):
        return lax.dot_general(
            factor,
            value,
            (((0,), (0,)), ((), ())),
            precision=high,
            preferred_element_type=jnp.float32,
        )

    normal = normalise(unit, window)
    own_window = normalise(unit_mixed, listed)
    inverse_tile = lax.psum_scatter(
        product(normal, ancestor_inverse, local_ids), "col", scatter_dimension=0, tiled=True
    )
    crossed = -lax.dot_general(
        own_window, inverse_tile, NT, precision=high, preferred_element_type=jnp.float32
    )
    parts = lax.all_to_all(
        crossed.reshape(width // pivot_inverse.shape[0], *pivot_inverse.shape), "row", 0, 0
    )
    diagonal_block = pivot_inverse + jnp.sum(parts, axis=0)
    return (inverse_tile, diagonal_block)


def table_kernel(cols, range_blocks, row_blocks, per_shard, ids_ref, slot_ref, block_ref, live_ref):
    c = lax.axis_index("col")
    slots = slot_ref.shape[1]
    quarter = row_blocks // cols
    for at in range(slots):
        for field in range(3):
            slot_ref[field, at] = 0
    for at in range(block_ref.shape[1]):
        for field in range(2):
            block_ref[field, at] = 0
    for at in range(live_ref.shape[0]):
        live_ref[at] = 0.0

    def step(k, rank):
        block = ids_ref[k]
        shard = k // per_shard
        offset = k % per_shard
        local = block - c * range_blocks
        here = (local >= 0) & (local < range_blocks)

        @pl.when(here)
        def _():
            slot_ref[0, rank] = shard
            slot_ref[1, rank] = offset
            slot_ref[2, rank] = local
            live_ref[rank] = 1.0

        row = block // row_blocks
        within = block % row_blocks

        @pl.when(within // quarter == c)
        def _():
            at = row * quarter + within % quarter
            block_ref[0, at] = shard
            block_ref[1, at] = offset
            live_ref[slots + at] = 1.0

        return rank + here.astype(jnp.int32)

    lax.fori_loop(0, ids_ref.shape[0], step, jnp.int32(0))


def tables(ids, cols, range_blocks, row_blocks, rows):
    smem = pl.BlockSpec(memory_space=pltpu.SMEM)
    quarter = row_blocks // cols
    return pl.pallas_call(
        functools.partial(
            table_kernel, cols, range_blocks, row_blocks, ids.shape[0] // cols
        ),
        out_shape=(
            jax.ShapeDtypeStruct((3, range_blocks // 2), jnp.int32),
            jax.ShapeDtypeStruct((2, rows * quarter), jnp.int32),
            jax.ShapeDtypeStruct((range_blocks // 2 + rows * quarter,), jnp.float32),
        ),
        in_specs=[smem],
        out_specs=(smem, smem, smem),
    )(ids)


def dot(a, b, dims):
    return lax.dot_general(a, b, dims, preferred_element_type=jnp.float32)


def dot3(a, b, dims):
    a_high, a_low = a
    b_high, b_low = b
    return dot(a_high, b_high, dims) + (dot(a_high, b_low, dims) + dot(a_low, b_high, dims))


PARTS = 4
A_TILES = 6


def remote(src, dst, send, recv, device):
    return pltpu.make_async_remote_copy(
        src_ref=src,
        dst_ref=dst,
        send_sem=send,
        recv_sem=recv,
        device_id=device,
        device_id_type=MESH,
    )


def fused_kernel(rows, cols, slot_ref, block_ref, live_ref, pt_ref, u_ref, pivot_ref, a_ref, *refs):
    out_ref, diag_ref = refs[:2]
    gathered = refs[2 : 2 + PARTS]
    stage = refs[2 + PARTS : 4 + PARTS]
    (
        pt, packed, a_high, a_low, m_ref, r1, r2, final, uf, ut_high, ut_low,
        ph_send, ph_recv, nh_high, nh_low, cit, qp, qc, qb, qd, qz,
        a_sem, ag_s, ag_r, up_s, up_r, dn_s, dn_r, core_s, core_r, u_s, u_r,
        ph_s, ph_r, r1_s, r1_r, r2_s, r2_r, out_s, out_r, qc_s, qc_r,
        qb_s, qb_r, qz_s, qz_r,
    ) = refs[4 + PARTS :]
    nz = rows // 2
    kw, width = u_ref.shape
    sub = kw // PARTS
    rows_here, cols_here = a_ref.shape
    slots = slot_ref.shape[1]
    chosen = slots * BLK
    rq = rows_here // cols
    hq = rq // 2
    wq = width // cols
    quarter = rq // BLK
    tile_rows = rows_here // A_TILES

    r, c = lax.axis_index("row"), lax.axis_index("col")
    z, p = r // 2, r % 2
    mate = r + 1 - 2 * p
    xc = c + 1 - 2 * (c % 2)
    yc = c + 2 - 4 * (c // 2)
    dc = 3 - c
    plane = (xc, yc, dc)

    def a_copy(t):
        return pltpu.make_async_copy(
            a_ref.at[pl.ds(t * tile_rows, tile_rows), :], stage[t % 2], a_sem.at[t % 2]
        )

    a_copy(0).start()
    a_copy(1).start()

    barrier = pltpu.get_barrier_semaphore()
    for step in range(1, rows):
        pl.semaphore_signal(
            barrier, inc=1, device_id=((r + step) % rows, c), device_id_type=MESH
        )
    for other in plane:
        pl.semaphore_signal(barrier, inc=1, device_id=(r, other), device_id_type=MESH)
    pl.semaphore_wait(barrier, rows - 1 + cols - 1)

    sent = []

    def start(copy, when=None):
        sent.append((copy, when))
        if when is None:
            copy.start()
        else:
            pl.when(when)(copy.start)

    for h in range(PARTS):
        for i, other in enumerate(plane):
            start(
                remote(
                    pt_ref.at[pl.ds(h * sub, sub), :],
                    gathered[h].at[c],
                    ag_s.at[h, i],
                    ag_r.at[h, i],
                    (r, other),
                )
            )
    for step in range(1, rows):
        start(remote(u_ref, uf.at[r], u_s.at[step], u_r.at[step], ((r + step) % rows, c)))
    uf[r] = u_ref[...]
    for h in range(PARTS):
        gathered[h][c] = pt_ref[pl.ds(h * sub, sub), :]

    def prepare(t):
        a_copy(t).wait()
        for s in range(slots):
            column = slot_ref[2, s] * BLK
            high, low = halves(stage[t % 2][:, pl.ds(column, BLK)])
            a_high[pl.ds(t * tile_rows, tile_rows), s * BLK : (s + 1) * BLK] = high
            a_low[pl.ds(t * tile_rows, tile_rows), s * BLK : (s + 1) * BLK] = low
        if t + 2 < A_TILES:
            a_copy(t + 2).start()

    def part(h):
        return pl.ds(h * sub, sub)

    def z_copy(source, h, d, up):
        send, recv = (up_s, up_r) if up else (dn_s, dn_r)
        target = r + 2 if up else r - 2
        where = pt.at[source, part(h), :]
        return remote(where, where, send.at[d, h], recv.at[d, h], (target, c))

    def core_copy(source, h):
        where = pt.at[source, part(h), :]
        return remote(where, where, core_s.at[source // 2, h], core_r.at[source // 2, h], (mate, c))

    def own_part(h):
        for i, other in enumerate(plane):
            remote(
                pt_ref.at[part(h), :], gathered[h].at[other], ag_s.at[h, i], ag_r.at[h, i],
                (r, other),
            ).wait_recv()
        for s in range(slots):
            offset = slot_ref[1, s] * BLK
            value = gathered[h][slot_ref[0, s], :, pl.ds(offset, BLK)]
            pt[r, part(h), s * BLK : (s + 1) * BLK] = value * live_ref[s]
        start(z_copy(r, h, 0, True), z < nz - 1)
        start(z_copy(r, h, 0, False), z > 0)
        start(core_copy(r, h))

    def tick(d, h):
        for up in (True, False):
            source = r - 2 * d if up else r + 2 * d
            there = (source >= 0) & (source < rows)
            onward = there & ((z < nz - 1) if up else (z > 0))
            pl.when(there)(lambda: z_copy(source, h, d - 1, up).wait_recv())
            if d < nz - 1:
                start(z_copy(source, h, d, up), onward)
            start(core_copy(source, h), there)

    def chip_at(j):
        near = jnp.where(z <= nz - 1 - z, z, nz - 1 - z)
        hop = (j + 1) // 2
        paired = z + hop if j % 2 else z - hop
        single = jnp.where(z <= nz - 1 - z, j, nz - 1 - j)
        return jnp.where(j <= 2 * near, paired, single)

    def pack(j):
        chip = chip_at(j)
        for h in range(PARTS):
            source = 2 * chip + 1 - p
            where = pt.at[source, part(h), :]
            remote(where, where, core_s.at[chip, h], core_r.at[chip, h], (mate, c)).wait_recv()
        for core in range(2):
            high, low = halves(pt[2 * chip + core])
            packed[core * kw : (core + 1) * kw, :] = high
            packed[(2 + core) * kw : (3 + core) * kw, :] = low

    def multiply(j, q, half):
        at = pl.ds(pl.multiple_of(q * rq + half * hq, 8), hq)
        both = dot(a_high[at, :], packed[...], NT)
        cross = dot(a_low[at, :], packed[: 2 * kw, :], NT)
        m_ref[j, at, :] = both[:, : 2 * kw] + (both[:, 2 * kw :] + cross)

    def tiles(q, half):
        return pl.ds(pl.multiple_of(q * rq + half * hq, 8), hq)

    first = ((xc, 0, xc, 0), (yc, 1, yc, 0), (dc, 0, xc, 1), (dc, 1, yc, 1))
    later = ((yc, 0), (xc, 1), (c, 0), (c, 1))

    def r1_copy(j, i):
        q, half, other, slot = first[i]
        return remote(
            m_ref.at[j, tiles(q, half), :],
            r1.at[j, half, slot],
            r1_s.at[j, half, slot],
            r1_r.at[j, half, slot],
            (r, other),
        )

    def r2_copy(j, half):
        return remote(
            r1.at[j, half, 1], r2.at[j, half], r2_s.at[j, half], r2_r.at[j, half],
            (r, xc if half else yc),
        )

    def product_tile(j, i):
        if i < 4:
            q, half, _, _ = first[i]
        else:
            q, half = later[i - 4]
        multiply(j, q, half)
        if i < 4:
            start(r1_copy(j, i))

    def reduce_first(j):
        for half in range(2):
            for i in range(4):
                if first[i][1] == half and first[i][3] == 1:
                    r1_copy(j, i).wait_recv()
            r1[j, half, 1] = r1[j, half, 1] + m_ref[j, tiles(xc if half else yc, half), :]
            start(r2_copy(j, half))

    def reduce_last(j):
        lanes = pl.ds(pl.multiple_of(chip_at(j) * 2 * kw, BLK), 2 * kw)
        for half in range(2):
            for i in range(4):
                if first[i][1] == half and first[i][3] == 0:
                    r1_copy(j, i).wait_recv()
            r2_copy(j, half).wait_recv()
            final[half * hq : (half + 1) * hq, lanes] = (
                m_ref[j, tiles(c, half), :] + r1[j, half, 0] + r2[j, half]
            )

    def listed_part(h):
        for target in range(rows):
            for k in range(quarter):
                at = target * quarter + k
                offset = block_ref[1, at] * BLK
                value = gathered[h][block_ref[0, at], :, pl.ds(offset, BLK)]
                ph_send[target, part(h), k * BLK : (k + 1) * BLK] = (
                    value * live_ref[slots + at]
                )

    def listed_send():
        for step in range(1, rows):
            target = (r + step) % rows
            start(
                remote(
                    ph_send.at[target], ph_recv.at[r], ph_s.at[step], ph_r.at[step], (target, c)
                )
            )
        ph_recv[r] = ph_send[r]

    def turn_unit():
        for step in range(1, rows):
            source = (r - step + rows) % rows
            remote(u_ref, uf.at[source], u_s.at[step], u_r.at[step], (r, c)).wait_recv()
        for chip in range(nz):
            both = jnp.concatenate([uf[2 * chip], uf[2 * chip + 1]], axis=0)
            high, low = halves(both.T)
            ut_high[:, chip * 2 * kw : (chip + 1) * 2 * kw] = high
            ut_low[:, chip * 2 * kw : (chip + 1) * 2 * kw] = low

    def normalise_listed():
        for step in range(1, rows):
            source = (r - step + rows) % rows
            remote(
                ph_send.at[source], ph_recv.at[source], ph_s.at[step], ph_r.at[step], (r, c)
            ).wait_recv()
        value = halves(ph_recv[...].reshape(width, rq))
        high, low = halves(dot3((ut_high[...], ut_low[...]), value, NN))
        nh_high[...] = high
        nh_low[...] = low

    for t in range(A_TILES - 2):
        prepare(t)
    for h in range(PARTS):
        own_part(h)
        if h < 2:
            prepare(A_TILES - 2 + h)

    for j in range(nz):
        pack(j)
        for h in range(PARTS):
            product_tile(j, 2 * h)
            product_tile(j, 2 * h + 1)
            if j + 1 < nz:
                tick(j + 1, h)
            if j == 0:
                listed_part(h)
            if h == 1 and j >= 1:
                reduce_first(j - 1)
        if j >= 2:
            reduce_last(j - 2)
        if j == 1:
            listed_send()
            turn_unit()
        if j == 2:
            normalise_listed()
    reduce_first(nz - 1)
    reduce_last(nz - 2)
    reduce_last(nz - 1)

    f_halves = halves(final[...])
    result = -dot3((ut_high[...], ut_low[...]), f_halves, NT)
    cit[...] = result

    def out_copy(i, other, source):
        return remote(
            cit.at[pl.ds(pl.multiple_of(other * wq, 8), wq), :],
            out_ref.at[:, pl.ds(pl.multiple_of(source * rq, BLK), rq)],
            out_s.at[i],
            out_r.at[i],
            (r, other),
        )

    for i, other in enumerate(plane):
        start(out_copy(i, other, c))

    ci = halves(result)
    for chip in range(nz):
        at = slice(chip * 2 * kw, (chip + 1) * 2 * kw)
        value = dot3((nh_high[at, :], nh_low[at, :]), ci, NT)
        qp[0, chip] = value[:kw]
        qp[1, chip] = value[kw:]
    core_sum = remote(qp.at[1 - p], qc, qc_s, qc_r, (mate, c))
    start(core_sum)
    out_ref[:, pl.ds(pl.multiple_of(c * rq, BLK), rq)] = cit[pl.ds(pl.multiple_of(c * wq, 8), wq), :]
    core_sum.wait_recv()
    qc[...] = qc[...] + qp[p]

    def lanes_of(column):
        return pl.ds(pl.multiple_of(column * wq, BLK), wq)

    def plane_copy(i, other):
        return remote(qc.at[:, :, lanes_of(other)], qb.at[i], qb_s.at[i], qb_r.at[i], (r, other))

    for i, other in enumerate(plane):
        start(plane_copy(i, other))
    for i, other in enumerate(plane):
        plane_copy(i, other).wait_recv()
    qd[...] = qc[:, :, lanes_of(c)] + (qb[0] + (qb[1] + qb[2]))
    for step in range(1, nz):
        target = (z + step) % nz
        start(
            remote(
                qd.at[target], qz.at[step], qz_s.at[step], qz_r.at[step], (2 * target + p, c)
            )
        )
    for step in range(1, nz):
        remote(qd.at[step], qz.at[step], qz_s.at[step], qz_r.at[step], (r, c)).wait_recv()
    total = qd[z]
    for step in range(1, nz):
        total = total + qz[step]
    diag_ref[...] = pivot_ref[...] - total

    for i, other in enumerate(plane):
        out_copy(i, other, other).wait_recv()
    for copy, when in sent:
        if when is None:
            copy.wait_send()
        else:
            pl.when(when)(copy.wait_send)


def fused(rows, cols, ancestor_inverse, panel, unit_inverse, pivot_inverse, panel_blocks):
    rows_here, cols_here = ancestor_inverse.shape
    stored, kw = panel.shape
    width = unit_inverse.shape[1]
    row_blocks, range_blocks = rows_here // BLK, cols_here // BLK
    slot_ids, block_ids, live = tables(panel_blocks, cols, range_blocks, row_blocks, rows)
    slots = range_blocks // 2
    chosen = slots * BLK
    nz = rows // 2
    rq, wq = rows_here // cols, width // cols
    f32, bf16 = jnp.float32, jnp.bfloat16
    dma = pltpu.SemaphoreType.DMA
    vmem = pl.BlockSpec(memory_space=pltpu.VMEM)
    smem = pl.BlockSpec(memory_space=pltpu.SMEM)
    scratch = (
        [pltpu.VMEM((cols, kw // PARTS, stored), f32)] * PARTS
        + [pltpu.VMEM((rows_here // A_TILES, cols_here), f32)] * 2
        + [
            pltpu.VMEM((rows, kw, chosen), f32),
            pltpu.VMEM((4 * kw, chosen), bf16),
            pltpu.VMEM((rows_here, chosen), bf16),
            pltpu.VMEM((rows_here, chosen), bf16),
            pltpu.VMEM((nz, rows_here, 2 * kw), f32),
            pltpu.VMEM((nz, 2, 2, rq // 2, 2 * kw), f32),
            pltpu.VMEM((nz, 2, rq // 2, 2 * kw), f32),
            pltpu.VMEM((rq, width), f32),
            pltpu.VMEM((rows, kw, width), f32),
            pltpu.VMEM((width, width), bf16),
            pltpu.VMEM((width, width), bf16),
            pltpu.VMEM((rows, kw, rq), f32),
            pltpu.VMEM((rows, kw, rq), f32),
            pltpu.VMEM((width, rq), bf16),
            pltpu.VMEM((width, rq), bf16),
            pltpu.VMEM((width, rq), f32),
            pltpu.VMEM((2, nz, kw, width), f32),
            pltpu.VMEM((nz, kw, width), f32),
            pltpu.VMEM((cols - 1, nz, kw, wq), f32),
            pltpu.VMEM((nz, kw, wq), f32),
            pltpu.VMEM((nz, kw, wq), f32),
            dma((2,)),
            dma((PARTS, cols - 1)),
            dma((PARTS, cols - 1)),
            dma((nz, PARTS)),
            dma((nz, PARTS)),
            dma((nz, PARTS)),
            dma((nz, PARTS)),
            dma((nz, PARTS)),
            dma((nz, PARTS)),
            dma((rows,)),
            dma((rows,)),
            dma((rows,)),
            dma((rows,)),
            dma((nz, 2, 2)),
            dma((nz, 2, 2)),
            dma((nz, 2)),
            dma((nz, 2)),
            dma((cols - 1,)),
            dma((cols - 1,)),
            dma,
            dma,
            dma((cols - 1,)),
            dma((cols - 1,)),
            dma((nz,)),
            dma((nz,)),
        ]
    )
    return pl.pallas_call(
        functools.partial(fused_kernel, rows, cols),
        out_shape=(
            jax.ShapeDtypeStruct((wq, rows_here), f32),
            jax.ShapeDtypeStruct(pivot_inverse.shape, f32),
        ),
        in_specs=[smem, smem, smem, vmem, vmem, vmem, pl.BlockSpec(memory_space=pl.ANY)],
        out_specs=(vmem, vmem),
        scratch_shapes=scratch,
        compiler_params=pltpu.CompilerParams(
            collective_id=0, has_side_effects=True, vmem_limit_bytes=62 << 20
        ),
    )(slot_ids, block_ids, live, panel.T, unit_inverse, pivot_inverse, ancestor_inverse)


def fits(mesh, ancestor_inverse, panel, unit_inverse):
    rows, cols = mesh.shape["row"], mesh.shape["col"]
    rows_here = ancestor_inverse.shape[0] // rows
    width = unit_inverse.shape[1]
    return (
        cols == 4
        and rows % 2 == 0
        and rows_here % (cols * BLK) == 0
        and rows_here % (16 * A_TILES) == 0
        and width == BLK * (rows // 2)
        and panel.shape[0] % (cols * BLK) == 0
        and ancestor_inverse.shape[1] % (2 * cols * BLK) == 0
    )


def solution(mesh):
    rows, cols = mesh.shape["row"], mesh.shape["col"]

    def whole(ancestor_inverse, panel, unit_inverse, pivot_inverse, panel_blocks):
        body = on_device
        if fits(mesh, ancestor_inverse, panel, unit_inverse):
            body = functools.partial(fused, rows, cols)
        return jax.shard_map(
            body,
            mesh=mesh,
            in_specs=(P("row", "col"), P("col", "row"), P("row", None), P("row", "col"), P()),
            out_specs=(P("col", "row"), P("row", "col")),
            check_vma=False,
        )(ancestor_inverse, panel, unit_inverse, pivot_inverse, panel_blocks)

    return whole
```

```python
import functools

import jax
import jax.numpy as jnp
from jax import lax
from jax.experimental import pallas as pl
from jax.experimental.pallas import tpu as pltpu
from jax.sharding import PartitionSpec as P

BLK = 128
NT = (((1,), (1,)), ((), ()))
NN = (((1,), (0,)), ((), ()))
MESH = pl.DeviceIdType.MESH


def select_kernel(per_shard, ids_ref, live_ref, gathered_ref, out_ref):
    slots = out_ref.shape[2] // BLK
    for target in range(out_ref.shape[0]):
        for slot in range(slots):
            at = target * slots + slot
            block = ids_ref[at]
            start = pl.multiple_of((block % per_shard) * BLK, BLK)
            value = gathered_ref[block // per_shard, :, pl.ds(start, BLK)]
            out_ref[target, :, slot * BLK : (slot + 1) * BLK] = jnp.where(
                live_ref[at] > 0, value, 0.0
            )


def select(gathered, ids, live, targets):
    slots = ids.shape[0] // targets
    per_shard = gathered.shape[2] // BLK
    smem = pl.BlockSpec(memory_space=pltpu.SMEM)
    vmem = pl.BlockSpec(memory_space=pltpu.VMEM)
    return pl.pallas_call(
        functools.partial(select_kernel, per_shard),
        out_shape=jax.ShapeDtypeStruct((targets, gathered.shape[1], slots * BLK), jnp.float32),
        in_specs=[smem, smem, vmem],
        out_specs=vmem,
    )(ids, live, gathered)


def halves(value):
    high = value.astype(jnp.bfloat16)
    return high, (value - high.astype(jnp.float32)).astype(jnp.bfloat16)


def product_kernel(group, ids_ref, normal_ref, *refs):
    out_ref = refs[group]

    @pl.when(pl.program_id(1) == 0)
    def _():
        out_ref[...] = jnp.zeros_like(out_ref)

    n_high, n_low = halves(normal_ref[...])
    if group == 1:
        block = refs[0][...]
    else:
        block = jnp.concatenate([ref[...] for ref in refs[:group]], axis=1)
    a_high, a_low = halves(block)
    dot = functools.partial(
        lax.dot_general, dimension_numbers=NT, preferred_element_type=jnp.float32
    )
    out_ref[...] -= dot(n_high, a_high) + (dot(n_high, a_low) + dot(n_low, a_high))


def product(normal, ancestor, ids):
    width, slots = normal.shape[0], ids.shape[0]
    rows = ancestor.shape[0]
    group = 2 if slots % 2 == 0 else 1
    tile = 512 if rows % 512 == 0 else BLK

    def column(k):
        return pl.BlockSpec((tile, BLK), lambda i, j, ids: (i, ids[j * group + k]))

    return pl.pallas_call(
        functools.partial(product_kernel, group),
        out_shape=jax.ShapeDtypeStruct((width, rows), jnp.float32),
        grid_spec=pltpu.PrefetchScalarGridSpec(
            num_scalar_prefetch=1,
            grid=(rows // tile, slots // group),
            in_specs=[pl.BlockSpec((width, group * BLK), lambda i, j, ids: (0, j))]
            + [column(k) for k in range(group)],
            out_specs=pl.BlockSpec((width, tile), lambda i, j, ids: (0, i)),
        ),
        compiler_params=pltpu.CompilerParams(
            dimension_semantics=("arbitrary", "arbitrary"), vmem_limit_bytes=32 << 20
        ),
        cost_estimate=pl.CostEstimate(
            flops=6 * width * rows * slots * BLK,
            bytes_accessed=4 * (rows * slots * BLK + 2 * width * rows),
            transcendentals=0,
        ),
    )(ids, normal, *([ancestor] * group))


def on_device(ancestor_inverse, panel, unit_inverse, pivot_inverse, panel_blocks):
    high = lax.Precision.HIGH
    col_index = lax.axis_index("col")
    rows_here, cols_here = ancestor_inverse.shape
    width = unit_inverse.shape[1]
    block_total = panel_blocks.shape[0]
    range_blocks = cols_here // BLK
    row_blocks = rows_here // BLK
    first_block = col_index * range_blocks
    slot_count = range_blocks // 2

    gathered = lax.all_gather(panel.T, "col", axis=0, tiled=False)
    half = width // 2
    unit = [
        lax.all_gather(unit_inverse[:, k * half : (k + 1) * half], "row", axis=0, tiled=True)
        for k in range(2)
    ]

    in_range = (panel_blocks >= first_block) & (panel_blocks < first_block + range_blocks)
    order = jnp.arange(block_total, dtype=jnp.int32)
    upto = order[None, :] <= order[:, None]
    rank_of = jnp.sum((upto & in_range[None, :]).astype(jnp.int32), axis=1) - 1
    slot_ids = jnp.arange(slot_count, dtype=jnp.int32)
    selected = in_range[None, :] & (rank_of[None, :] == slot_ids[:, None])
    stored_ids = jnp.sum(jnp.where(selected, order[None, :], 0), axis=1)
    chosen_ids = jnp.sum(jnp.where(selected, panel_blocks[None, :], 0), axis=1)
    slot_live = jnp.sum(selected.astype(jnp.int32), axis=1)
    local_ids = jnp.clip(chosen_ids - first_block, 0, range_blocks - 1)
    gathered, unit = lax.optimization_barrier((gathered, unit))
    unit = jnp.concatenate(unit, axis=1)
    rows, cols = lax.axis_size("row"), lax.axis_size("col")
    chosen = select(gathered, stored_ids, slot_live, 1)[0]
    window = lax.all_gather(chosen, "row", axis=0, tiled=True)

    match = panel_blocks[None, :] == jnp.arange(rows * row_blocks, dtype=jnp.int32)[:, None]
    block_ids = jnp.sum(jnp.where(match, order[None, :], 0), axis=1)
    block_live = jnp.sum(match.astype(jnp.int32), axis=1)
    part = panel.shape[1] // cols
    share = lax.dynamic_slice_in_dim(gathered, col_index * part, part, 1)
    listed = lax.all_to_all(select(share, block_ids, block_live, rows), "row", 0, 0)
    listed = lax.all_gather(listed, "col", axis=0, tiled=False).reshape(width, rows_here)
    unit_mixed = unit.reshape(rows, cols, part, width).transpose(1, 0, 2, 3).reshape(width, width)

    def normalise(factor, value):
        return lax.dot_general(
            factor,
            value,
            (((0,), (0,)), ((), ())),
            precision=high,
            preferred_element_type=jnp.float32,
        )

    normal = normalise(unit, window)
    own_window = normalise(unit_mixed, listed)
    inverse_tile = lax.psum_scatter(
        product(normal, ancestor_inverse, local_ids), "col", scatter_dimension=0, tiled=True
    )
    crossed = -lax.dot_general(
        own_window, inverse_tile, NT, precision=high, preferred_element_type=jnp.float32
    )
    parts = lax.all_to_all(
        crossed.reshape(width // pivot_inverse.shape[0], *pivot_inverse.shape), "row", 0, 0
    )
    diagonal_block = pivot_inverse + jnp.sum(parts, axis=0)
    return (inverse_tile, diagonal_block)


def table_kernel(cols, range_blocks, row_blocks, per_shard, ids_ref, slot_ref, block_ref, live_ref):
    c = lax.axis_index("col")
    slots = slot_ref.shape[1]
    quarter = row_blocks // cols
    for at in range(slots):
        for field in range(3):
            slot_ref[field, at] = 0
    for at in range(block_ref.shape[1]):
        for field in range(2):
            block_ref[field, at] = 0
    for at in range(live_ref.shape[0]):
        live_ref[at] = 0.0

    def step(k, rank):
        block = ids_ref[k]
        shard = k // per_shard
        offset = k % per_shard
        local = block - c * range_blocks
        here = (local >= 0) & (local < range_blocks)

        @pl.when(here)
        def _():
            slot_ref[0, rank] = shard
            slot_ref[1, rank] = offset
            slot_ref[2, rank] = local
            live_ref[rank] = 1.0

        row = block // row_blocks
        within = block % row_blocks

        @pl.when(within // quarter == c)
        def _():
            at = row * quarter + within % quarter
            block_ref[0, at] = shard
            block_ref[1, at] = offset
            live_ref[slots + at] = 1.0

        return rank + here.astype(jnp.int32)

    lax.fori_loop(0, ids_ref.shape[0], step, jnp.int32(0))


def tables(ids, cols, range_blocks, row_blocks, rows):
    smem = pl.BlockSpec(memory_space=pltpu.SMEM)
    quarter = row_blocks // cols
    return pl.pallas_call(
        functools.partial(
            table_kernel, cols, range_blocks, row_blocks, ids.shape[0] // cols
        ),
        out_shape=(
            jax.ShapeDtypeStruct((3, range_blocks // 2), jnp.int32),
            jax.ShapeDtypeStruct((2, rows * quarter), jnp.int32),
            jax.ShapeDtypeStruct((range_blocks // 2 + rows * quarter,), jnp.float32),
        ),
        in_specs=[smem],
        out_specs=(smem, smem, smem),
    )(ids)


def dot(a, b, dims):
    return lax.dot_general(a, b, dims, preferred_element_type=jnp.float32)


def dot3(a, b, dims):
    a_high, a_low = a
    b_high, b_low = b
    return dot(a_high, b_high, dims) + (dot(a_high, b_low, dims) + dot(a_low, b_high, dims))


PARTS = 4
A_TILES = 6


def remote(src, dst, send, recv, device):
    return pltpu.make_async_remote_copy(
        src_ref=src,
        dst_ref=dst,
        send_sem=send,
        recv_sem=recv,
        device_id=device,
        device_id_type=MESH,
    )


def fused_kernel(rows, cols, slot_ref, block_ref, live_ref, pt_ref, u_ref, pivot_ref, a_ref, *refs):
    out_ref, diag_ref = refs[:2]
    gathered = refs[2 : 2 + PARTS]
    stage = refs[2 + PARTS : 4 + PARTS]
    (
        pt, packed, a_high, a_low, m_ref, r1, r2, final, uf, ut_high, ut_low,
        ph_send, ph_recv, nh_high, nh_low, cit, qp, qc, qb, qd, qz,
        a_sem, ag_s, ag_r, up_s, up_r, dn_s, dn_r, core_s, core_r, uu_s, uu_r, ud_s, ud_r, um_s, um_r,
        ph_s, ph_r, r1_s, r1_r, r2_s, r2_r, out_s, out_r, qc_s, qc_r,
        qb_s, qb_r, qz_s, qz_r,
    ) = refs[4 + PARTS :]
    nz = rows // 2
    kw, width = u_ref.shape
    sub = kw // PARTS
    rows_here, cols_here = a_ref.shape
    slots = slot_ref.shape[1]
    chosen = slots * BLK
    rq = rows_here // cols
    hq = rq // 2
    wq = width // cols
    quarter = rq // BLK
    tile_rows = rows_here // A_TILES

    r, c = lax.axis_index("row"), lax.axis_index("col")
    z, p = r // 2, r % 2
    mate = r + 1 - 2 * p
    xc = c + 1 - 2 * (c % 2)
    yc = c + 2 - 4 * (c // 2)
    dc = 3 - c
    plane = (xc, yc, dc)

    def a_copy(t):
        return pltpu.make_async_copy(
            a_ref.at[pl.ds(t * tile_rows, tile_rows), :], stage[t % 2], a_sem.at[t % 2]
        )

    a_copy(0).start()
    a_copy(1).start()

    barrier = pltpu.get_barrier_semaphore()
    for step in range(1, rows):
        pl.semaphore_signal(
            barrier, inc=1, device_id=((r + step) % rows, c), device_id_type=MESH
        )
    for other in plane:
        pl.semaphore_signal(barrier, inc=1, device_id=(r, other), device_id_type=MESH)
    pl.semaphore_wait(barrier, rows - 1 + cols - 1)

    sent = []

    def start(copy, when=None):
        sent.append((copy, when))
        if when is None:
            copy.start()
        else:
            pl.when(when)(copy.start)

    def part(h):
        return pl.ds(h * sub, sub)

    def own_copy(h, i, source):
        return remote(
            pt_ref.at[part(h), :],
            gathered[h].at[source],
            ag_s.at[h, i],
            ag_r.at[h, i],
            (r, plane[i]),
        )

    def own_send(h):
        for i in range(cols - 1):
            start(own_copy(h, i, c))

    own_send(0)
    def unit_copy(source, chip, d, up):
        send, recv = (uu_s, uu_r) if up else (ud_s, ud_r)
        where = uf.at[source, :, pl.ds(0, 2 * kw * (chip + 1))]
        data = u_ref.at[:, pl.ds(0, 2 * kw * (chip + 1))] if d == 0 else where
        return remote(data, where, send.at[d], recv.at[d], (r + 2 if up else r - 2, c))

    def unit_mate(source):
        where = uf.at[source]
        return remote(where, where, um_s.at[source // 2], um_r.at[source // 2], (mate, c))

    for chip in range(nz):
        if chip < nz - 1:
            start(unit_copy(r, chip, 0, True), z == chip)
        if chip > 0:
            start(unit_copy(r, chip, 0, False), z == chip)
    for chip in range(nz - 1):
        uf[2 * chip + p, :, 2 * kw * (chip + 1) :] = jnp.zeros(
            (kw, width - 2 * kw * (chip + 1)), jnp.float32
        )
    own_unit = remote(u_ref, uf.at[r], um_s.at[z], um_r.at[z], (mate, c))
    start(own_unit)

    def unit_tick(d):
        for up in (True, False):
            source = r - 2 * d if up else r + 2 * d
            for chip in range(nz):
                at = z - d == chip if up else z + d == chip
                onward = at & ((z < nz - 1) if up else (z > 0))
                pl.when(at)(unit_copy(source, chip, d - 1, up).wait_recv)
                if d < nz - 1:
                    start(unit_copy(source, chip, d, up), onward)
            start(unit_mate(source), (source >= 0) & (source < rows))

    for h in range(PARTS):
        gathered[h][c] = pt_ref[part(h), :]

    def prepare(t):
        a_copy(t).wait()
        for s in range(slots):
            column = slot_ref[2, s] * BLK
            high, low = halves(stage[t % 2][:, pl.ds(column, BLK)])
            a_high[pl.ds(t * tile_rows, tile_rows), s * BLK : (s + 1) * BLK] = high
            a_low[pl.ds(t * tile_rows, tile_rows), s * BLK : (s + 1) * BLK] = low
        if t + 2 < A_TILES:
            a_copy(t + 2).start()

    def z_copy(source, h, d, up):
        send, recv = (up_s, up_r) if up else (dn_s, dn_r)
        target = r + 2 if up else r - 2
        where = pt.at[source, part(h), :]
        return remote(where, where, send.at[d, h], recv.at[d, h], (target, c))

    def core_copy(source, h):
        where = pt.at[source, part(h), :]
        return remote(where, where, core_s.at[source // 2, h], core_r.at[source // 2, h], (mate, c))

    def own_part(h):
        for i in range(cols - 1):
            own_copy(h, i, plane[i]).wait_recv()
        for s in range(slots):
            offset = slot_ref[1, s] * BLK
            value = gathered[h][slot_ref[0, s], :, pl.ds(offset, BLK)]
            pt[r, part(h), s * BLK : (s + 1) * BLK] = value * live_ref[s]
        start(z_copy(r, h, 0, True), z < nz - 1)
        start(z_copy(r, h, 0, False), z > 0)
        start(core_copy(r, h))

    def tick(d, h):
        for up in (True, False):
            source = r - 2 * d if up else r + 2 * d
            there = (source >= 0) & (source < rows)
            onward = there & ((z < nz - 1) if up else (z > 0))
            pl.when(there)(lambda: z_copy(source, h, d - 1, up).wait_recv())
            if d < nz - 1:
                start(z_copy(source, h, d, up), onward)
            start(core_copy(source, h), there)

    def chip_at(j):
        near = jnp.where(z <= nz - 1 - z, z, nz - 1 - z)
        hop = (j + 1) // 2
        paired = z + hop if j % 2 else z - hop
        single = jnp.where(z <= nz - 1 - z, j, nz - 1 - j)
        return jnp.where(j <= 2 * near, paired, single)

    def pack(j):
        chip = chip_at(j)
        for h in range(PARTS):
            source = 2 * chip + 1 - p
            where = pt.at[source, part(h), :]
            remote(where, where, core_s.at[chip, h], core_r.at[chip, h], (mate, c)).wait_recv()
        for core in range(2):
            high, low = halves(pt[2 * chip + core])
            packed[core * kw : (core + 1) * kw, :] = high
            packed[(2 + core) * kw : (3 + core) * kw, :] = low

    def multiply(j, q, half):
        at = pl.ds(pl.multiple_of(q * rq + half * hq, 8), hq)
        both = dot(a_high[at, :], packed[...], NT)
        cross = dot(a_low[at, :], packed[: 2 * kw, :], NT)
        m_ref[j, at, :] = both[:, : 2 * kw] + (both[:, 2 * kw :] + cross)

    def tiles(q, half):
        return pl.ds(pl.multiple_of(q * rq + half * hq, 8), hq)

    first = ((xc, 0, xc, 0), (yc, 1, yc, 0), (dc, 0, xc, 1), (dc, 1, yc, 1))
    later = ((yc, 0), (xc, 1), (c, 0), (c, 1))

    def r1_copy(j, i):
        q, half, other, slot = first[i]
        return remote(
            m_ref.at[j, tiles(q, half), :],
            r1.at[j, half, slot],
            r1_s.at[j, half, slot],
            r1_r.at[j, half, slot],
            (r, other),
        )

    def r2_copy(j, half):
        return remote(
            r1.at[j, half, 1], r2.at[j, half], r2_s.at[j, half], r2_r.at[j, half],
            (r, xc if half else yc),
        )

    def product_tile(j, i):
        if i < 4:
            q, half, _, _ = first[i]
        else:
            q, half = later[i - 4]
        multiply(j, q, half)
        if i < 4:
            start(r1_copy(j, i))

    def reduce_first(j):
        for half in range(2):
            for i in range(4):
                if first[i][1] == half and first[i][3] == 1:
                    r1_copy(j, i).wait_recv()
            r1[j, half, 1] = r1[j, half, 1] + m_ref[j, tiles(xc if half else yc, half), :]
            start(r2_copy(j, half))

    def reduce_last(j):
        lanes = pl.ds(pl.multiple_of(chip_at(j) * 2 * kw, BLK), 2 * kw)
        for half in range(2):
            for i in range(4):
                if first[i][1] == half and first[i][3] == 0:
                    r1_copy(j, i).wait_recv()
            r2_copy(j, half).wait_recv()
            final[half * hq : (half + 1) * hq, lanes] = (
                m_ref[j, tiles(c, half), :] + r1[j, half, 0] + r2[j, half]
            )

    def listed_part(h):
        for target in range(rows):
            for k in range(quarter):
                at = target * quarter + k
                offset = block_ref[1, at] * BLK
                value = gathered[h][block_ref[0, at], :, pl.ds(offset, BLK)]
                ph_send[target, part(h), k * BLK : (k + 1) * BLK] = (
                    value * live_ref[slots + at]
                )

    def listed_send():
        for step in range(1, rows):
            target = (r + step) % rows
            start(
                remote(
                    ph_send.at[target], ph_recv.at[r], ph_s.at[step], ph_r.at[step], (target, c)
                )
            )
        ph_recv[r] = ph_send[r]

    def turn_unit():
        uf[r] = u_ref[...]
        for chip in range(nz):
            unit_mate(2 * chip + 1 - p).wait_recv()
        for chip in range(nz):
            both = jnp.concatenate([uf[2 * chip], uf[2 * chip + 1]], axis=0)
            high, low = halves(both.T)
            ut_high[:, chip * 2 * kw : (chip + 1) * 2 * kw] = high
            ut_low[:, chip * 2 * kw : (chip + 1) * 2 * kw] = low

    def normalise_listed():
        for step in range(1, rows):
            source = (r - step + rows) % rows
            remote(
                ph_send.at[source], ph_recv.at[source], ph_s.at[step], ph_r.at[step], (r, c)
            ).wait_recv()
        value = halves(ph_recv[...].reshape(width, rq))
        high, low = halves(dot3((ut_high[...], ut_low[...]), value, NN))
        nh_high[...] = high
        nh_low[...] = low

    def out_copy(i, other, source):
        return remote(
            cit.at[pl.ds(pl.multiple_of(other * wq, 8), wq), :],
            out_ref.at[:, pl.ds(pl.multiple_of(source * rq, BLK), rq)],
            out_s.at[i],
            out_r.at[i],
            (r, other),
        )

    def unit_product():
        cit[...] = -dot3((ut_high[...], ut_low[...]), halves(final[...]), NT)
        for i, other in enumerate(plane):
            start(out_copy(i, other, c))
        out_ref[:, pl.ds(pl.multiple_of(c * rq, BLK), rq)] = cit[
            pl.ds(pl.multiple_of(c * wq, 8), wq), :
        ]

    core_sum = remote(qp.at[1 - p], qc, qc_s, qc_r, (mate, c))

    def listed_product():
        ci = halves(cit[...])
        for chip in range(nz):
            at = slice(chip * 2 * kw, (chip + 1) * 2 * kw)
            value = dot3((nh_high[at, :], nh_low[at, :]), ci, NT)
            qp[0, chip] = value[:kw]
            qp[1, chip] = value[kw:]
        start(core_sum)

    def lanes_of(column):
        return pl.ds(pl.multiple_of(column * wq, BLK), wq)

    def plane_copy(i, other):
        return remote(qc.at[:, :, lanes_of(other)], qb.at[i], qb_s.at[i], qb_r.at[i], (r, other))

    def sum_cores():
        core_sum.wait_recv()
        qc[...] = qc[...] + qp[p]
        for i, other in enumerate(plane):
            start(plane_copy(i, other))

    def sum_plane():
        for i, other in enumerate(plane):
            plane_copy(i, other).wait_recv()
        qd[...] = qc[:, :, lanes_of(c)] + (qb[0] + (qb[1] + qb[2]))
        for step in range(1, nz):
            target = (z + step) % nz
            start(
                remote(
                    qd.at[target], qz.at[step], qz_s.at[step], qz_r.at[step], (2 * target + p, c)
                )
            )

    def sum_line():
        for step in range(1, nz):
            remote(qd.at[step], qz.at[step], qz_s.at[step], qz_r.at[step], (r, c)).wait_recv()
        total = qd[z]
        for step in range(1, nz):
            total = total + qz[step]
        diag_ref[...] = pivot_ref[...] - total

    def finish():
        for i, other in enumerate(plane):
            out_copy(i, other, other).wait_recv()
        for copy, when in sent:
            if when is None:
                copy.wait_send()
            else:
                pl.when(when)(copy.wait_send)

    prepare(0)
    prepare(1)
    prepare(2)
    prepare(3)
    own_send(1)
    unit_tick(1)
    prepare(4)
    own_part(0)
    own_send(2)
    unit_tick(2)
    prepare(5)
    own_part(1)
    own_send(3)
    tick(1, 0)
    own_part(2)
    tick(1, 1)
    own_part(3)
    tick(2, 0)
    unit_tick(3)
    tick(1, 2)

    between = {
        (0, 1): (2, 1), (0, 3): (1, 3), (0, 7): (2, 2), (1, 1): (2, 3), (1, 4): (3, 0),
        (1, 7): (3, 1), (2, 2): (3, 2), (2, 5): (3, 3),
    }
    for j in range(nz):
        pack(j)
        for i in range(8):
            product_tile(j, i)
            if (j, i) in between:
                tick(*between[j, i])
            if j == 0 and i == 4:
                for h in range(PARTS):
                    listed_part(h)
            if j == 1 and i == 4:
                turn_unit()
            if j >= 1 and i == 4:
                reduce_first(j - 1)
            if j >= 2 and i == 6:
                reduce_last(j - 2)
        if j == nz - 2:
            listed_send()
    reduce_first(nz - 1)
    reduce_last(nz - 2)
    reduce_last(nz - 1)
    unit_product()
    normalise_listed()
    listed_product()
    sum_cores()
    sum_plane()
    sum_line()
    finish()


def fused(rows, cols, ancestor_inverse, panel, unit_inverse, pivot_inverse, panel_blocks):
    rows_here, cols_here = ancestor_inverse.shape
    stored, kw = panel.shape
    width = unit_inverse.shape[1]
    row_blocks, range_blocks = rows_here // BLK, cols_here // BLK
    slot_ids, block_ids, live = tables(panel_blocks, cols, range_blocks, row_blocks, rows)
    slots = range_blocks // 2
    chosen = slots * BLK
    nz = rows // 2
    rq, wq = rows_here // cols, width // cols
    f32, bf16 = jnp.float32, jnp.bfloat16
    dma = pltpu.SemaphoreType.DMA
    vmem = pl.BlockSpec(memory_space=pltpu.VMEM)
    smem = pl.BlockSpec(memory_space=pltpu.SMEM)
    scratch = (
        [pltpu.VMEM((cols, kw // PARTS, stored), f32)] * PARTS
        + [pltpu.VMEM((rows_here // A_TILES, cols_here), f32)] * 2
        + [
            pltpu.VMEM((rows, kw, chosen), f32),
            pltpu.VMEM((4 * kw, chosen), bf16),
            pltpu.VMEM((rows_here, chosen), bf16),
            pltpu.VMEM((rows_here, chosen), bf16),
            pltpu.VMEM((nz, rows_here, 2 * kw), f32),
            pltpu.VMEM((nz, 2, 2, rq // 2, 2 * kw), f32),
            pltpu.VMEM((nz, 2, rq // 2, 2 * kw), f32),
            pltpu.VMEM((rq, width), f32),
            pltpu.VMEM((rows, kw, width), f32),
            pltpu.VMEM((width, width), bf16),
            pltpu.VMEM((width, width), bf16),
            pltpu.VMEM((rows, kw, rq), f32),
            pltpu.VMEM((rows, kw, rq), f32),
            pltpu.VMEM((width, rq), bf16),
            pltpu.VMEM((width, rq), bf16),
            pltpu.VMEM((width, rq), f32),
            pltpu.VMEM((2, nz, kw, width), f32),
            pltpu.VMEM((nz, kw, width), f32),
            pltpu.VMEM((cols - 1, nz, kw, wq), f32),
            pltpu.VMEM((nz, kw, wq), f32),
            pltpu.VMEM((nz, kw, wq), f32),
            dma((2,)),
            dma((PARTS, cols - 1)),
            dma((PARTS, cols - 1)),
            dma((nz, PARTS)),
            dma((nz, PARTS)),
            dma((nz, PARTS)),
            dma((nz, PARTS)),
            dma((nz, PARTS)),
            dma((nz, PARTS)),
            dma((nz,)),
            dma((nz,)),
            dma((nz,)),
            dma((nz,)),
            dma((nz,)),
            dma((nz,)),
            dma((rows,)),
            dma((rows,)),
            dma((nz, 2, 2)),
            dma((nz, 2, 2)),
            dma((nz, 2)),
            dma((nz, 2)),
            dma((cols - 1,)),
            dma((cols - 1,)),
            dma,
            dma,
            dma((cols - 1,)),
            dma((cols - 1,)),
            dma((nz,)),
            dma((nz,)),
        ]
    )
    return pl.pallas_call(
        functools.partial(fused_kernel, rows, cols),
        out_shape=(
            jax.ShapeDtypeStruct((wq, rows_here), f32),
            jax.ShapeDtypeStruct(pivot_inverse.shape, f32),
        ),
        in_specs=[smem, smem, smem, vmem, vmem, vmem, pl.BlockSpec(memory_space=pl.ANY)],
        out_specs=(vmem, vmem),
        scratch_shapes=scratch,
        compiler_params=pltpu.CompilerParams(
            collective_id=0, has_side_effects=True, vmem_limit_bytes=62 << 20
        ),
    )(slot_ids, block_ids, live, panel.T, unit_inverse, pivot_inverse, ancestor_inverse)


def fits(mesh, ancestor_inverse, panel, unit_inverse):
    rows, cols = mesh.shape["row"], mesh.shape["col"]
    rows_here = ancestor_inverse.shape[0] // rows
    width = unit_inverse.shape[1]
    return (
        cols == 4
        and rows % 2 == 0
        and rows_here % (cols * BLK) == 0
        and rows_here % (16 * A_TILES) == 0
        and width == BLK * (rows // 2)
        and panel.shape[0] % (cols * BLK) == 0
        and ancestor_inverse.shape[1] % (2 * cols * BLK) == 0
    )


def solution(mesh):
    rows, cols = mesh.shape["row"], mesh.shape["col"]

    def whole(ancestor_inverse, panel, unit_inverse, pivot_inverse, panel_blocks):
        body = on_device
        if fits(mesh, ancestor_inverse, panel, unit_inverse):
            body = functools.partial(fused, rows, cols)
        return jax.shard_map(
            body,
            mesh=mesh,
            in_specs=(P("row", "col"), P("col", "row"), P("row", None), P("row", "col"), P()),
            out_specs=(P("col", "row"), P("row", "col")),
            check_vma=False,
        )(ancestor_inverse, panel, unit_inverse, pivot_inverse, panel_blocks)

    return whole
```

```python
import functools

import jax
import jax.numpy as jnp
from jax import lax
from jax.experimental import pallas as pl
from jax.experimental.pallas import tpu as pltpu
from jax.sharding import PartitionSpec as P

BLK = 128
NT = (((1,), (1,)), ((), ()))
NN = (((1,), (0,)), ((), ()))
MESH = pl.DeviceIdType.MESH


def select_kernel(per_shard, ids_ref, live_ref, gathered_ref, out_ref):
    slots = out_ref.shape[2] // BLK
    for target in range(out_ref.shape[0]):
        for slot in range(slots):
            at = target * slots + slot
            block = ids_ref[at]
            start = pl.multiple_of((block % per_shard) * BLK, BLK)
            value = gathered_ref[block // per_shard, :, pl.ds(start, BLK)]
            out_ref[target, :, slot * BLK : (slot + 1) * BLK] = jnp.where(
                live_ref[at] > 0, value, 0.0
            )


def select(gathered, ids, live, targets):
    slots = ids.shape[0] // targets
    per_shard = gathered.shape[2] // BLK
    smem = pl.BlockSpec(memory_space=pltpu.SMEM)
    vmem = pl.BlockSpec(memory_space=pltpu.VMEM)
    return pl.pallas_call(
        functools.partial(select_kernel, per_shard),
        out_shape=jax.ShapeDtypeStruct((targets, gathered.shape[1], slots * BLK), jnp.float32),
        in_specs=[smem, smem, vmem],
        out_specs=vmem,
    )(ids, live, gathered)


def halves(value):
    high = value.astype(jnp.bfloat16)
    return high, (value - high.astype(jnp.float32)).astype(jnp.bfloat16)


def product_kernel(group, ids_ref, normal_ref, *refs):
    out_ref = refs[group]

    @pl.when(pl.program_id(1) == 0)
    def _():
        out_ref[...] = jnp.zeros_like(out_ref)

    n_high, n_low = halves(normal_ref[...])
    if group == 1:
        block = refs[0][...]
    else:
        block = jnp.concatenate([ref[...] for ref in refs[:group]], axis=1)
    a_high, a_low = halves(block)
    dot = functools.partial(
        lax.dot_general, dimension_numbers=NT, preferred_element_type=jnp.float32
    )
    out_ref[...] -= dot(n_high, a_high) + (dot(n_high, a_low) + dot(n_low, a_high))


def product(normal, ancestor, ids):
    width, slots = normal.shape[0], ids.shape[0]
    rows = ancestor.shape[0]
    group = 2 if slots % 2 == 0 else 1
    tile = 512 if rows % 512 == 0 else BLK

    def column(k):
        return pl.BlockSpec((tile, BLK), lambda i, j, ids: (i, ids[j * group + k]))

    return pl.pallas_call(
        functools.partial(product_kernel, group),
        out_shape=jax.ShapeDtypeStruct((width, rows), jnp.float32),
        grid_spec=pltpu.PrefetchScalarGridSpec(
            num_scalar_prefetch=1,
            grid=(rows // tile, slots // group),
            in_specs=[pl.BlockSpec((width, group * BLK), lambda i, j, ids: (0, j))]
            + [column(k) for k in range(group)],
            out_specs=pl.BlockSpec((width, tile), lambda i, j, ids: (0, i)),
        ),
        compiler_params=pltpu.CompilerParams(
            dimension_semantics=("arbitrary", "arbitrary"), vmem_limit_bytes=32 << 20
        ),
        cost_estimate=pl.CostEstimate(
            flops=6 * width * rows * slots * BLK,
            bytes_accessed=4 * (rows * slots * BLK + 2 * width * rows),
            transcendentals=0,
        ),
    )(ids, normal, *([ancestor] * group))


def on_device(ancestor_inverse, panel, unit_inverse, pivot_inverse, panel_blocks):
    high = lax.Precision.HIGH
    col_index = lax.axis_index("col")
    rows_here, cols_here = ancestor_inverse.shape
    width = unit_inverse.shape[1]
    block_total = panel_blocks.shape[0]
    range_blocks = cols_here // BLK
    row_blocks = rows_here // BLK
    first_block = col_index * range_blocks
    slot_count = range_blocks // 2

    gathered = lax.all_gather(panel.T, "col", axis=0, tiled=False)
    half = width // 2
    unit = [
        lax.all_gather(unit_inverse[:, k * half : (k + 1) * half], "row", axis=0, tiled=True)
        for k in range(2)
    ]

    in_range = (panel_blocks >= first_block) & (panel_blocks < first_block + range_blocks)
    order = jnp.arange(block_total, dtype=jnp.int32)
    upto = order[None, :] <= order[:, None]
    rank_of = jnp.sum((upto & in_range[None, :]).astype(jnp.int32), axis=1) - 1
    slot_ids = jnp.arange(slot_count, dtype=jnp.int32)
    selected = in_range[None, :] & (rank_of[None, :] == slot_ids[:, None])
    stored_ids = jnp.sum(jnp.where(selected, order[None, :], 0), axis=1)
    chosen_ids = jnp.sum(jnp.where(selected, panel_blocks[None, :], 0), axis=1)
    slot_live = jnp.sum(selected.astype(jnp.int32), axis=1)
    local_ids = jnp.clip(chosen_ids - first_block, 0, range_blocks - 1)
    gathered, unit = lax.optimization_barrier((gathered, unit))
    unit = jnp.concatenate(unit, axis=1)
    rows, cols = lax.axis_size("row"), lax.axis_size("col")
    chosen = select(gathered, stored_ids, slot_live, 1)[0]
    window = lax.all_gather(chosen, "row", axis=0, tiled=True)

    match = panel_blocks[None, :] == jnp.arange(rows * row_blocks, dtype=jnp.int32)[:, None]
    block_ids = jnp.sum(jnp.where(match, order[None, :], 0), axis=1)
    block_live = jnp.sum(match.astype(jnp.int32), axis=1)
    part = panel.shape[1] // cols
    share = lax.dynamic_slice_in_dim(gathered, col_index * part, part, 1)
    listed = lax.all_to_all(select(share, block_ids, block_live, rows), "row", 0, 0)
    listed = lax.all_gather(listed, "col", axis=0, tiled=False).reshape(width, rows_here)
    unit_mixed = unit.reshape(rows, cols, part, width).transpose(1, 0, 2, 3).reshape(width, width)

    def normalise(factor, value):
        return lax.dot_general(
            factor,
            value,
            (((0,), (0,)), ((), ())),
            precision=high,
            preferred_element_type=jnp.float32,
        )

    normal = normalise(unit, window)
    own_window = normalise(unit_mixed, listed)
    inverse_tile = lax.psum_scatter(
        product(normal, ancestor_inverse, local_ids), "col", scatter_dimension=0, tiled=True
    )
    crossed = -lax.dot_general(
        own_window, inverse_tile, NT, precision=high, preferred_element_type=jnp.float32
    )
    parts = lax.all_to_all(
        crossed.reshape(width // pivot_inverse.shape[0], *pivot_inverse.shape), "row", 0, 0
    )
    diagonal_block = pivot_inverse + jnp.sum(parts, axis=0)
    return (inverse_tile, diagonal_block)


def table_kernel(cols, range_blocks, row_blocks, per_shard, ids_ref, slot_ref, block_ref, live_ref):
    c = lax.axis_index("col")
    slots = slot_ref.shape[1]
    quarter = row_blocks // cols
    for at in range(slots):
        for field in range(3):
            slot_ref[field, at] = 0
    for at in range(block_ref.shape[1]):
        for field in range(2):
            block_ref[field, at] = 0
    for at in range(live_ref.shape[0]):
        live_ref[at] = 0.0

    def step(k, rank):
        block = ids_ref[k]
        shard = k // per_shard
        offset = k % per_shard
        local = block - c * range_blocks
        here = (local >= 0) & (local < range_blocks)

        @pl.when(here)
        def _():
            slot_ref[0, rank] = shard
            slot_ref[1, rank] = offset
            slot_ref[2, rank] = local
            live_ref[rank] = 1.0

        row = block // row_blocks
        within = block % row_blocks

        @pl.when(within // quarter == c)
        def _():
            at = row * quarter + within % quarter
            block_ref[0, at] = shard
            block_ref[1, at] = offset
            live_ref[slots + at] = 1.0

        return rank + here.astype(jnp.int32)

    lax.fori_loop(0, ids_ref.shape[0], step, jnp.int32(0))


def tables(ids, cols, range_blocks, row_blocks, rows):
    smem = pl.BlockSpec(memory_space=pltpu.SMEM)
    quarter = row_blocks // cols
    return pl.pallas_call(
        functools.partial(
            table_kernel, cols, range_blocks, row_blocks, ids.shape[0] // cols
        ),
        out_shape=(
            jax.ShapeDtypeStruct((3, range_blocks // 2), jnp.int32),
            jax.ShapeDtypeStruct((2, rows * quarter), jnp.int32),
            jax.ShapeDtypeStruct((range_blocks // 2 + rows * quarter,), jnp.float32),
        ),
        in_specs=[smem],
        out_specs=(smem, smem, smem),
    )(ids)


def dot(a, b, dims):
    return lax.dot_general(a, b, dims, preferred_element_type=jnp.float32)


def dot3(a, b, dims):
    a_high, a_low = a
    b_high, b_low = b
    return dot(a_high, b_high, dims) + (dot(a_high, b_low, dims) + dot(a_low, b_high, dims))


PARTS = 4
A_TILES = 6


def remote(src, dst, send, recv, device):
    return pltpu.make_async_remote_copy(
        src_ref=src,
        dst_ref=dst,
        send_sem=send,
        recv_sem=recv,
        device_id=device,
        device_id_type=MESH,
    )


def fused_kernel(rows, cols, slot_ref, block_ref, live_ref, pt_ref, u_ref, pivot_ref, a_ref, *refs):
    out_ref, diag_ref = refs[:2]
    gathered = refs[2 : 2 + PARTS]
    stage = refs[2 + PARTS : 4 + PARTS]
    (
        pt, packed, a_high, a_low, m_ref, r1, r2, final, uf, ut_high, ut_low,
        ph_send, ph_recv, nh_high, nh_low, cit, qp, qc, qb, qd, qz,
        a_sem, ag_s, ag_r, up_s, up_r, dn_s, dn_r, core_s, core_r, uu_s, uu_r, ud_s, ud_r, um_s, um_r,
        ph_s, ph_r, r1_s, r1_r, r2_s, r2_r, out_s, out_r, qc_s, qc_r,
        qb_s, qb_r, qz_s, qz_r,
    ) = refs[4 + PARTS :]
    nz = rows // 2
    kw, width = u_ref.shape
    sub = kw // PARTS
    rows_here, cols_here = a_ref.shape
    slots = slot_ref.shape[1]
    chosen = slots * BLK
    rq = rows_here // cols
    hq = rq // 2
    wq = width // cols
    quarter = rq // BLK
    tile_rows = rows_here // A_TILES

    r, c = lax.axis_index("row"), lax.axis_index("col")
    z, p = r // 2, r % 2
    mate = r + 1 - 2 * p
    xc = c + 1 - 2 * (c % 2)
    yc = c + 2 - 4 * (c // 2)
    dc = 3 - c
    plane = (xc, yc, dc)

    def a_copy(t):
        return pltpu.make_async_copy(
            a_ref.at[pl.ds(t * tile_rows, tile_rows), :], stage[t % 2], a_sem.at[t % 2]
        )

    a_copy(0).start()
    a_copy(1).start()

    barrier = pltpu.get_barrier_semaphore()
    for step in range(1, rows):
        pl.semaphore_signal(
            barrier, inc=1, device_id=((r + step) % rows, c), device_id_type=MESH
        )
    for other in plane:
        pl.semaphore_signal(barrier, inc=1, device_id=(r, other), device_id_type=MESH)
    pl.semaphore_wait(barrier, rows - 1 + cols - 1)

    sent = []

    def start(copy, when=None):
        sent.append((copy, when))
        if when is None:
            copy.start()
        else:
            pl.when(when)(copy.start)

    def part(h):
        return pl.ds(h * sub, sub)

    def own_copy(h, i, source):
        return remote(
            pt_ref.at[part(h), :],
            gathered[h].at[source],
            ag_s.at[h, i],
            ag_r.at[h, i],
            (r, plane[i]),
        )

    def own_send(h):
        for i in range(cols - 1):
            start(own_copy(h, i, c))

    own_send(0)
    def unit_copy(source, chip, d, up):
        send, recv = (uu_s, uu_r) if up else (ud_s, ud_r)
        where = uf.at[source, :, pl.ds(0, 2 * kw * (chip + 1))]
        data = u_ref.at[:, pl.ds(0, 2 * kw * (chip + 1))] if d == 0 else where
        return remote(data, where, send.at[d], recv.at[d], (r + 2 if up else r - 2, c))

    def unit_mate(source):
        where = uf.at[source]
        return remote(where, where, um_s.at[source // 2], um_r.at[source // 2], (mate, c))

    for chip in range(nz):
        if chip < nz - 1:
            start(unit_copy(r, chip, 0, True), z == chip)
        if chip > 0:
            start(unit_copy(r, chip, 0, False), z == chip)
    for chip in range(nz - 1):
        uf[2 * chip + p, :, 2 * kw * (chip + 1) :] = jnp.zeros(
            (kw, width - 2 * kw * (chip + 1)), jnp.float32
        )
    own_unit = remote(u_ref, uf.at[r], um_s.at[z], um_r.at[z], (mate, c))
    start(own_unit)

    def unit_tick(d):
        for up in (True, False):
            source = r - 2 * d if up else r + 2 * d
            for chip in range(nz):
                at = z - d == chip if up else z + d == chip
                onward = at & ((z < nz - 1) if up else (z > 0))
                pl.when(at)(unit_copy(source, chip, d - 1, up).wait_recv)
                if d < nz - 1:
                    start(unit_copy(source, chip, d, up), onward)
            start(unit_mate(source), (source >= 0) & (source < rows))

    for h in range(PARTS):
        gathered[h][c] = pt_ref[part(h), :]

    def prepare(t):
        a_copy(t).wait()
        for s in range(slots):
            column = slot_ref[2, s] * BLK
            high, low = halves(stage[t % 2][:, pl.ds(column, BLK)])
            a_high[pl.ds(t * tile_rows, tile_rows), s * BLK : (s + 1) * BLK] = high
            a_low[pl.ds(t * tile_rows, tile_rows), s * BLK : (s + 1) * BLK] = low
        if t + 2 < A_TILES:
            a_copy(t + 2).start()

    def z_copy(source, h, d, up):
        send, recv = (up_s, up_r) if up else (dn_s, dn_r)
        target = r + 2 if up else r - 2
        where = pt.at[source, part(h), :]
        return remote(where, where, send.at[d, h], recv.at[d, h], (target, c))

    def core_copy(source, h):
        where = pt.at[source, part(h), :]
        return remote(where, where, core_s.at[source // 2, h], core_r.at[source // 2, h], (mate, c))

    def own_part(h):
        for i in range(cols - 1):
            own_copy(h, i, plane[i]).wait_recv()
        for s in range(slots):
            offset = slot_ref[1, s] * BLK
            value = gathered[h][slot_ref[0, s], :, pl.ds(offset, BLK)]
            pt[r, part(h), s * BLK : (s + 1) * BLK] = value * live_ref[s]
        start(z_copy(r, h, 0, True), z < nz - 1)
        start(z_copy(r, h, 0, False), z > 0)
        start(core_copy(r, h))

    def tick(d, h):
        for up in (True, False):
            source = r - 2 * d if up else r + 2 * d
            there = (source >= 0) & (source < rows)
            onward = there & ((z < nz - 1) if up else (z > 0))
            pl.when(there)(lambda: z_copy(source, h, d - 1, up).wait_recv())
            if d < nz - 1:
                start(z_copy(source, h, d, up), onward)
            start(core_copy(source, h), there)

    def chip_at(j):
        near = jnp.where(z <= nz - 1 - z, z, nz - 1 - z)
        hop = (j + 1) // 2
        paired = z + hop if j % 2 else z - hop
        single = jnp.where(z <= nz - 1 - z, j, nz - 1 - j)
        return jnp.where(j <= 2 * near, paired, single)

    def pack(j):
        chip = chip_at(j)
        for h in range(PARTS):
            source = 2 * chip + 1 - p
            where = pt.at[source, part(h), :]
            remote(where, where, core_s.at[chip, h], core_r.at[chip, h], (mate, c)).wait_recv()
        for core in range(2):
            high, low = halves(pt[2 * chip + core])
            packed[core * kw : (core + 1) * kw, :] = high
            packed[(2 + core) * kw : (3 + core) * kw, :] = low

    def multiply(j, q, half):
        at = pl.ds(pl.multiple_of(q * rq + half * hq, 8), hq)
        both = dot(a_high[at, :], packed[...], NT)
        cross = dot(a_low[at, :], packed[: 2 * kw, :], NT)
        m_ref[j, at, :] = both[:, : 2 * kw] + (both[:, 2 * kw :] + cross)

    def tiles(q, half):
        return pl.ds(pl.multiple_of(q * rq + half * hq, 8), hq)

    first = ((xc, 0, xc, 0), (yc, 1, yc, 0), (dc, 0, xc, 1), (dc, 1, yc, 1))
    later = ((yc, 0), (xc, 1), (c, 0), (c, 1))

    def r1_copy(j, i):
        q, half, other, slot = first[i]
        return remote(
            m_ref.at[j, tiles(q, half), :],
            r1.at[j, half, slot],
            r1_s.at[j, half, slot],
            r1_r.at[j, half, slot],
            (r, other),
        )

    def r2_copy(j, half):
        return remote(
            r1.at[j, half, 1], r2.at[j, half], r2_s.at[j, half], r2_r.at[j, half],
            (r, xc if half else yc),
        )

    def product_tile(j, i):
        if i < 4:
            q, half, _, _ = first[i]
        else:
            q, half = later[i - 4]
        multiply(j, q, half)
        if i < 4:
            start(r1_copy(j, i))

    def reduce_first(j):
        for half in range(2):
            for i in range(4):
                if first[i][1] == half and first[i][3] == 1:
                    r1_copy(j, i).wait_recv()
            r1[j, half, 1] = r1[j, half, 1] + m_ref[j, tiles(xc if half else yc, half), :]
            start(r2_copy(j, half))

    def reduce_last(j):
        lanes = pl.ds(pl.multiple_of(chip_at(j) * 2 * kw, BLK), 2 * kw)
        for half in range(2):
            for i in range(4):
                if first[i][1] == half and first[i][3] == 0:
                    r1_copy(j, i).wait_recv()
            r2_copy(j, half).wait_recv()
            final[half * hq : (half + 1) * hq, lanes] = (
                m_ref[j, tiles(c, half), :] + r1[j, half, 0] + r2[j, half]
            )

    def listed_part(h):
        for target in range(rows):
            for k in range(quarter):
                at = target * quarter + k
                offset = block_ref[1, at] * BLK
                value = gathered[h][block_ref[0, at], :, pl.ds(offset, BLK)]
                ph_send[target, part(h), k * BLK : (k + 1) * BLK] = (
                    value * live_ref[slots + at]
                )

    def listed_send():
        for step in range(1, rows):
            target = (r + step) % rows
            start(
                remote(
                    ph_send.at[target], ph_recv.at[r], ph_s.at[step], ph_r.at[step], (target, c)
                )
            )
        ph_recv[r] = ph_send[r]

    def turn_unit():
        uf[r] = u_ref[...]
        for chip in range(nz):
            unit_mate(2 * chip + 1 - p).wait_recv()
        for chip in range(nz):
            both = jnp.concatenate([uf[2 * chip], uf[2 * chip + 1]], axis=0)
            high, low = halves(both.T)
            ut_high[:, chip * 2 * kw : (chip + 1) * 2 * kw] = high
            ut_low[:, chip * 2 * kw : (chip + 1) * 2 * kw] = low

    def normalise_listed():
        for step in range(1, rows):
            source = (r - step + rows) % rows
            remote(
                ph_send.at[source], ph_recv.at[source], ph_s.at[step], ph_r.at[step], (r, c)
            ).wait_recv()
        value = halves(ph_recv[...].reshape(width, rq))
        high, low = halves(dot3((ut_high[...], ut_low[...]), value, NN))
        nh_high[...] = high
        nh_low[...] = low

    def out_copy(i, other, source):
        return remote(
            cit.at[pl.ds(pl.multiple_of(other * wq, 8), wq), :],
            out_ref.at[:, pl.ds(pl.multiple_of(source * rq, BLK), rq)],
            out_s.at[i],
            out_r.at[i],
            (r, other),
        )

    def unit_product():
        cit[...] = -dot3((ut_high[...], ut_low[...]), halves(final[...]), NT)
        for i, other in enumerate(plane):
            start(out_copy(i, other, c))
        out_ref[:, pl.ds(pl.multiple_of(c * rq, BLK), rq)] = cit[
            pl.ds(pl.multiple_of(c * wq, 8), wq), :
        ]

    core_sum = remote(qp.at[1 - p], qc, qc_s, qc_r, (mate, c))

    def listed_product():
        ci = halves(cit[...])
        for chip in range(nz):
            at = slice(chip * 2 * kw, (chip + 1) * 2 * kw)
            value = dot3((nh_high[at, :], nh_low[at, :]), ci, NT)
            qp[0, chip] = value[:kw]
            qp[1, chip] = value[kw:]
        start(core_sum)

    def lanes_of(column):
        return pl.ds(pl.multiple_of(column * wq, BLK), wq)

    def plane_copy(i, other):
        return remote(qc.at[:, :, lanes_of(other)], qb.at[i], qb_s.at[i], qb_r.at[i], (r, other))

    def sum_cores():
        core_sum.wait_recv()
        qc[...] = qc[...] + qp[p]
        for i, other in enumerate(plane):
            start(plane_copy(i, other))

    def sum_plane():
        for i, other in enumerate(plane):
            plane_copy(i, other).wait_recv()
        qd[...] = qc[:, :, lanes_of(c)] + (qb[0] + (qb[1] + qb[2]))
        for step in range(1, nz):
            target = (z + step) % nz
            start(
                remote(
                    qd.at[target], qz.at[step], qz_s.at[step], qz_r.at[step], (2 * target + p, c)
                )
            )

    def sum_line():
        for step in range(1, nz):
            remote(qd.at[step], qz.at[step], qz_s.at[step], qz_r.at[step], (r, c)).wait_recv()
        total = qd[z]
        for step in range(1, nz):
            total = total + qz[step]
        diag_ref[...] = pivot_ref[...] - total

    def finish():
        for i, other in enumerate(plane):
            out_copy(i, other, other).wait_recv()
        for copy, when in sent:
            if when is None:
                copy.wait_send()
            else:
                pl.when(when)(copy.wait_send)

    prepare(0)
    prepare(1)
    prepare(2)
    prepare(3)
    own_send(1)
    unit_tick(1)
    prepare(4)
    own_part(0)
    own_send(2)
    unit_tick(2)
    prepare(5)
    own_part(1)
    own_send(3)
    tick(1, 0)
    own_part(2)
    tick(1, 1)
    own_part(3)
    tick(2, 0)
    unit_tick(3)
    tick(1, 2)

    between = {
        (0, 1): (2, 1), (0, 3): (1, 3), (0, 7): (2, 2), (1, 7): (2, 3), (2, 1): (3, 0),
        (2, 3): (3, 1), (2, 5): (3, 2), (2, 7): (3, 3),
    }
    for j in range(nz):
        pack(j)
        if j == nz - 1:
            listed_send()
        for i in range(8):
            product_tile(j, i)
            if (j, i) in between:
                tick(*between[j, i])
            if j == 0 and i == 4:
                for h in range(PARTS):
                    listed_part(h)
            if j == 1 and i == 4:
                turn_unit()
            if j >= 1 and i == 4:
                reduce_first(j - 1)
            if j >= 2 and i == 6:
                reduce_last(j - 2)
    reduce_first(nz - 1)
    reduce_last(nz - 2)
    reduce_last(nz - 1)
    unit_product()
    normalise_listed()
    listed_product()
    sum_cores()
    sum_plane()
    sum_line()
    finish()


def fused(rows, cols, ancestor_inverse, panel, unit_inverse, pivot_inverse, panel_blocks):
    rows_here, cols_here = ancestor_inverse.shape
    stored, kw = panel.shape
    width = unit_inverse.shape[1]
    row_blocks, range_blocks = rows_here // BLK, cols_here // BLK
    slot_ids, block_ids, live = tables(panel_blocks, cols, range_blocks, row_blocks, rows)
    slots = range_blocks // 2
    chosen = slots * BLK
    nz = rows // 2
    rq, wq = rows_here // cols, width // cols
    f32, bf16 = jnp.float32, jnp.bfloat16
    dma = pltpu.SemaphoreType.DMA
    vmem = pl.BlockSpec(memory_space=pltpu.VMEM)
    smem = pl.BlockSpec(memory_space=pltpu.SMEM)
    scratch = (
        [pltpu.VMEM((cols, kw // PARTS, stored), f32)] * PARTS
        + [pltpu.VMEM((rows_here // A_TILES, cols_here), f32)] * 2
        + [
            pltpu.VMEM((rows, kw, chosen), f32),
            pltpu.VMEM((4 * kw, chosen), bf16),
            pltpu.VMEM((rows_here, chosen), bf16),
            pltpu.VMEM((rows_here, chosen), bf16),
            pltpu.VMEM((nz, rows_here, 2 * kw), f32),
            pltpu.VMEM((nz, 2, 2, rq // 2, 2 * kw), f32),
            pltpu.VMEM((nz, 2, rq // 2, 2 * kw), f32),
            pltpu.VMEM((rq, width), f32),
            pltpu.VMEM((rows, kw, width), f32),
            pltpu.VMEM((width, width), bf16),
            pltpu.VMEM((width, width), bf16),
            pltpu.VMEM((rows, kw, rq), f32),
            pltpu.VMEM((rows, kw, rq), f32),
            pltpu.VMEM((width, rq), bf16),
            pltpu.VMEM((width, rq), bf16),
            pltpu.VMEM((width, rq), f32),
            pltpu.VMEM((2, nz, kw, width), f32),
            pltpu.VMEM((nz, kw, width), f32),
            pltpu.VMEM((cols - 1, nz, kw, wq), f32),
            pltpu.VMEM((nz, kw, wq), f32),
            pltpu.VMEM((nz, kw, wq), f32),
            dma((2,)),
            dma((PARTS, cols - 1)),
            dma((PARTS, cols - 1)),
            dma((nz, PARTS)),
            dma((nz, PARTS)),
            dma((nz, PARTS)),
            dma((nz, PARTS)),
            dma((nz, PARTS)),
            dma((nz, PARTS)),
            dma((nz,)),
            dma((nz,)),
            dma((nz,)),
            dma((nz,)),
            dma((nz,)),
            dma((nz,)),
            dma((rows,)),
            dma((rows,)),
            dma((nz, 2, 2)),
            dma((nz, 2, 2)),
            dma((nz, 2)),
            dma((nz, 2)),
            dma((cols - 1,)),
            dma((cols - 1,)),
            dma,
            dma,
            dma((cols - 1,)),
            dma((cols - 1,)),
            dma((nz,)),
            dma((nz,)),
        ]
    )
    return pl.pallas_call(
        functools.partial(fused_kernel, rows, cols),
        out_shape=(
            jax.ShapeDtypeStruct((wq, rows_here), f32),
            jax.ShapeDtypeStruct(pivot_inverse.shape, f32),
        ),
        in_specs=[smem, smem, smem, vmem, vmem, vmem, pl.BlockSpec(memory_space=pl.ANY)],
        out_specs=(vmem, vmem),
        scratch_shapes=scratch,
        compiler_params=pltpu.CompilerParams(
            collective_id=0, has_side_effects=True, vmem_limit_bytes=50 << 20
        ),
    )(slot_ids, block_ids, live, panel.T, unit_inverse, pivot_inverse, ancestor_inverse)


def fits(mesh, ancestor_inverse, panel, unit_inverse):
    rows, cols = mesh.shape["row"], mesh.shape["col"]
    rows_here = ancestor_inverse.shape[0] // rows
    width = unit_inverse.shape[1]
    return (
        cols == 4
        and rows % 2 == 0
        and rows_here % (cols * BLK) == 0
        and rows_here % (16 * A_TILES) == 0
        and width == BLK * (rows // 2)
        and panel.shape[0] % (cols * BLK) == 0
        and ancestor_inverse.shape[1] % (2 * cols * BLK) == 0
    )


def solution(mesh):
    rows, cols = mesh.shape["row"], mesh.shape["col"]

    def whole(ancestor_inverse, panel, unit_inverse, pivot_inverse, panel_blocks):
        body = on_device
        if fits(mesh, ancestor_inverse, panel, unit_inverse):
            body = functools.partial(fused, rows, cols)
        return jax.shard_map(
            body,
            mesh=mesh,
            in_specs=(P("row", "col"), P("col", "row"), P("row", None), P("row", "col"), P()),
            out_specs=(P("col", "row"), P("row", "col")),
            check_vma=False,
        )(ancestor_inverse, panel, unit_inverse, pivot_inverse, panel_blocks)

    return whole
```

```python
import functools

import jax
import jax.numpy as jnp
from jax import lax
from jax.experimental import pallas as pl
from jax.experimental.pallas import tpu as pltpu
from jax.sharding import PartitionSpec as P

BLK = 128
NT = (((1,), (1,)), ((), ()))
NN = (((1,), (0,)), ((), ()))
MESH = pl.DeviceIdType.MESH


def select_kernel(per_shard, ids_ref, live_ref, gathered_ref, out_ref):
    slots = out_ref.shape[2] // BLK
    for target in range(out_ref.shape[0]):
        for slot in range(slots):
            at = target * slots + slot
            block = ids_ref[at]
            start = pl.multiple_of((block % per_shard) * BLK, BLK)
            value = gathered_ref[block // per_shard, :, pl.ds(start, BLK)]
            out_ref[target, :, slot * BLK : (slot + 1) * BLK] = jnp.where(
                live_ref[at] > 0, value, 0.0
            )


def select(gathered, ids, live, targets):
    slots = ids.shape[0] // targets
    per_shard = gathered.shape[2] // BLK
    smem = pl.BlockSpec(memory_space=pltpu.SMEM)
    vmem = pl.BlockSpec(memory_space=pltpu.VMEM)
    return pl.pallas_call(
        functools.partial(select_kernel, per_shard),
        out_shape=jax.ShapeDtypeStruct((targets, gathered.shape[1], slots * BLK), jnp.float32),
        in_specs=[smem, smem, vmem],
        out_specs=vmem,
    )(ids, live, gathered)


def halves(value):
    high = value.astype(jnp.bfloat16)
    return high, (value - high.astype(jnp.float32)).astype(jnp.bfloat16)


def product_kernel(group, ids_ref, normal_ref, *refs):
    out_ref = refs[group]

    @pl.when(pl.program_id(1) == 0)
    def _():
        out_ref[...] = jnp.zeros_like(out_ref)

    n_high, n_low = halves(normal_ref[...])
    if group == 1:
        block = refs[0][...]
    else:
        block = jnp.concatenate([ref[...] for ref in refs[:group]], axis=1)
    a_high, a_low = halves(block)
    dot = functools.partial(
        lax.dot_general, dimension_numbers=NT, preferred_element_type=jnp.float32
    )
    out_ref[...] -= dot(n_high, a_high) + (dot(n_high, a_low) + dot(n_low, a_high))


def product(normal, ancestor, ids):
    width, slots = normal.shape[0], ids.shape[0]
    rows = ancestor.shape[0]
    group = 2 if slots % 2 == 0 else 1
    tile = 512 if rows % 512 == 0 else BLK

    def column(k):
        return pl.BlockSpec((tile, BLK), lambda i, j, ids: (i, ids[j * group + k]))

    return pl.pallas_call(
        functools.partial(product_kernel, group),
        out_shape=jax.ShapeDtypeStruct((width, rows), jnp.float32),
        grid_spec=pltpu.PrefetchScalarGridSpec(
            num_scalar_prefetch=1,
            grid=(rows // tile, slots // group),
            in_specs=[pl.BlockSpec((width, group * BLK), lambda i, j, ids: (0, j))]
            + [column(k) for k in range(group)],
            out_specs=pl.BlockSpec((width, tile), lambda i, j, ids: (0, i)),
        ),
        compiler_params=pltpu.CompilerParams(
            dimension_semantics=("arbitrary", "arbitrary"), vmem_limit_bytes=32 << 20
        ),
        cost_estimate=pl.CostEstimate(
            flops=6 * width * rows * slots * BLK,
            bytes_accessed=4 * (rows * slots * BLK + 2 * width * rows),
            transcendentals=0,
        ),
    )(ids, normal, *([ancestor] * group))


def on_device(ancestor_inverse, panel, unit_inverse, pivot_inverse, panel_blocks):
    high = lax.Precision.HIGH
    col_index = lax.axis_index("col")
    rows_here, cols_here = ancestor_inverse.shape
    width = unit_inverse.shape[1]
    block_total = panel_blocks.shape[0]
    range_blocks = cols_here // BLK
    row_blocks = rows_here // BLK
    first_block = col_index * range_blocks
    slot_count = range_blocks // 2

    gathered = lax.all_gather(panel.T, "col", axis=0, tiled=False)
    half = width // 2
    unit = [
        lax.all_gather(unit_inverse[:, k * half : (k + 1) * half], "row", axis=0, tiled=True)
        for k in range(2)
    ]

    in_range = (panel_blocks >= first_block) & (panel_blocks < first_block + range_blocks)
    order = jnp.arange(block_total, dtype=jnp.int32)
    upto = order[None, :] <= order[:, None]
    rank_of = jnp.sum((upto & in_range[None, :]).astype(jnp.int32), axis=1) - 1
    slot_ids = jnp.arange(slot_count, dtype=jnp.int32)
    selected = in_range[None, :] & (rank_of[None, :] == slot_ids[:, None])
    stored_ids = jnp.sum(jnp.where(selected, order[None, :], 0), axis=1)
    chosen_ids = jnp.sum(jnp.where(selected, panel_blocks[None, :], 0), axis=1)
    slot_live = jnp.sum(selected.astype(jnp.int32), axis=1)
    local_ids = jnp.clip(chosen_ids - first_block, 0, range_blocks - 1)
    gathered, unit = lax.optimization_barrier((gathered, unit))
    unit = jnp.concatenate(unit, axis=1)
    rows, cols = lax.axis_size("row"), lax.axis_size("col")
    chosen = select(gathered, stored_ids, slot_live, 1)[0]
    window = lax.all_gather(chosen, "row", axis=0, tiled=True)

    match = panel_blocks[None, :] == jnp.arange(rows * row_blocks, dtype=jnp.int32)[:, None]
    block_ids = jnp.sum(jnp.where(match, order[None, :], 0), axis=1)
    block_live = jnp.sum(match.astype(jnp.int32), axis=1)
    part = panel.shape[1] // cols
    share = lax.dynamic_slice_in_dim(gathered, col_index * part, part, 1)
    listed = lax.all_to_all(select(share, block_ids, block_live, rows), "row", 0, 0)
    listed = lax.all_gather(listed, "col", axis=0, tiled=False).reshape(width, rows_here)
    unit_mixed = unit.reshape(rows, cols, part, width).transpose(1, 0, 2, 3).reshape(width, width)

    def normalise(factor, value):
        return lax.dot_general(
            factor,
            value,
            (((0,), (0,)), ((), ())),
            precision=high,
            preferred_element_type=jnp.float32,
        )

    normal = normalise(unit, window)
    own_window = normalise(unit_mixed, listed)
    inverse_tile = lax.psum_scatter(
        product(normal, ancestor_inverse, local_ids), "col", scatter_dimension=0, tiled=True
    )
    crossed = -lax.dot_general(
        own_window, inverse_tile, NT, precision=high, preferred_element_type=jnp.float32
    )
    parts = lax.all_to_all(
        crossed.reshape(width // pivot_inverse.shape[0], *pivot_inverse.shape), "row", 0, 0
    )
    diagonal_block = pivot_inverse + jnp.sum(parts, axis=0)
    return (inverse_tile, diagonal_block)


def table_kernel(cols, range_blocks, row_blocks, per_shard, ids_ref, table_ref):
    c = lax.axis_index("col")
    slots = range_blocks // 2
    quarter = row_blocks // cols
    for at in range(table_ref.shape[0]):
        table_ref[at] = 0

    def step(k, rank):
        block = ids_ref[k]
        shard = k // per_shard
        offset = k % per_shard
        local = block - c * range_blocks
        here = (local >= 0) & (local < range_blocks)

        @pl.when(here)
        def _():
            table_ref[rank] = shard
            table_ref[slots + rank] = offset
            table_ref[2 * slots + rank] = local
            table_ref[3 * slots + rank] = 1

        row = block // row_blocks
        within = block % row_blocks

        @pl.when(within // quarter == c)
        def _():
            at = row * quarter + within % quarter
            table_ref[4 * slots + 3 * at] = shard
            table_ref[4 * slots + 3 * at + 1] = offset
            table_ref[4 * slots + 3 * at + 2] = 1

        return rank + here.astype(jnp.int32)

    lax.fori_loop(0, ids_ref.shape[0], step, jnp.int32(0))


def tables(ids, cols, range_blocks, row_blocks, rows):
    smem = pl.BlockSpec(memory_space=pltpu.SMEM)
    quarter = row_blocks // cols
    return pl.pallas_call(
        functools.partial(
            table_kernel, cols, range_blocks, row_blocks, ids.shape[0] // cols
        ),
        out_shape=jax.ShapeDtypeStruct((2 * range_blocks + 3 * rows * quarter,), jnp.int32),
        in_specs=[smem],
        out_specs=smem,
    )(ids)


def dot(a, b, dims):
    return lax.dot_general(a, b, dims, preferred_element_type=jnp.float32)


def dot3(a, b, dims):
    a_high, a_low = a
    b_high, b_low = b
    return dot(a_high, b_high, dims) + (dot(a_high, b_low, dims) + dot(a_low, b_high, dims))


PARTS = 4
A_TILES = 6


def remote(src, dst, send, recv, device):
    return pltpu.make_async_remote_copy(
        src_ref=src,
        dst_ref=dst,
        send_sem=send,
        recv_sem=recv,
        device_id=device,
        device_id_type=MESH,
    )


def fused_kernel(rows, cols, table_ref, pt_ref, u_ref, pivot_hbm, a_ref, *refs):
    out_ref, diag_ref = refs[:2]
    gathered = refs[2 : 2 + PARTS]
    stage = refs[2 + PARTS : 4 + PARTS]
    (
        pt, packed, a_high, a_low, m_ref, r1, r2, final, uf, ut_high, ut_low,
        ph_send, ph_recv, nh_high, nh_low, cit, qp, qc, qb, qd, qz,
        unit_own, pivot_ref, in_sem, a_sem, ag_s, ag_r, up_s, up_r, dn_s, dn_r, core_s, core_r, uu_s, uu_r, ud_s, ud_r, um_s, um_r,
        ph_s, ph_r, r1_s, r1_r, r2_s, r2_r, out_s, out_r, qc_s, qc_r,
        qb_s, qb_r, qz_s, qz_r,
    ) = refs[4 + PARTS :]
    nz = rows // 2
    kw, width = u_ref.shape
    sub = kw // PARTS
    rows_here, cols_here = a_ref.shape
    slots = cols_here // BLK // 2
    rq = rows_here // cols
    hq = rq // 2
    wq = width // cols
    quarter = rq // BLK
    tile_rows = rows_here // A_TILES

    r, c = lax.axis_index("row"), lax.axis_index("col")
    z, p = r // 2, r % 2
    mate = r + 1 - 2 * p
    xc = c + 1 - 2 * (c % 2)
    yc = c + 2 - 4 * (c // 2)
    dc = 3 - c
    plane = (xc, yc, dc)

    def a_copy(t):
        return pltpu.make_async_copy(
            a_ref.at[pl.ds(t * tile_rows, tile_rows), :], stage[t % 2], a_sem.at[t % 2]
        )

    a_copy(0).start()
    a_copy(1).start()

    barrier = pltpu.get_barrier_semaphore()
    for step in range(1, rows):
        pl.semaphore_signal(
            barrier, inc=1, device_id=((r + step) % rows, c), device_id_type=MESH
        )
    for other in plane:
        pl.semaphore_signal(barrier, inc=1, device_id=(r, other), device_id_type=MESH)
    pl.semaphore_wait(barrier, rows - 1 + cols - 1)

    sent = []

    def start(copy, when=None):
        sent.append((copy, when))
        if when is None:
            copy.start()
        else:
            pl.when(when)(copy.start)

    def part(h):
        return pl.ds(h * sub, sub)

    def own_copy(h, i, source):
        return remote(
            pt_ref.at[part(h), :],
            gathered[h].at[source],
            ag_s.at[h, i],
            ag_r.at[h, i],
            (r, plane[i]),
        )

    def own_send(h):
        for i in range(cols - 1):
            start(own_copy(h, i, c))

    own_send(0)
    def unit_copy(source, chip, d, up):
        send, recv = (uu_s, uu_r) if up else (ud_s, ud_r)
        where = uf.at[source, :, pl.ds(0, 2 * kw * (chip + 1))]
        data = u_ref.at[:, pl.ds(0, 2 * kw * (chip + 1))] if d == 0 else where
        return remote(data, where, send.at[d], recv.at[d], (r + 2 if up else r - 2, c))

    def unit_mate(source):
        where = uf.at[source]
        return remote(where, where, um_s.at[source // 2], um_r.at[source // 2], (mate, c))

    for chip in range(nz):
        if chip < nz - 1:
            start(unit_copy(r, chip, 0, True), z == chip)
        if chip > 0:
            start(unit_copy(r, chip, 0, False), z == chip)
    for chip in range(nz - 1):
        uf[2 * chip + p, :, 2 * kw * (chip + 1) :] = jnp.zeros(
            (kw, width - 2 * kw * (chip + 1)), jnp.float32
        )
    own_unit = remote(u_ref, uf.at[r], um_s.at[z], um_r.at[z], (mate, c))
    start(own_unit)

    def unit_tick(d):
        for up in (True, False):
            source = r - 2 * d if up else r + 2 * d
            for chip in range(nz):
                at = z - d == chip if up else z + d == chip
                onward = at & ((z < nz - 1) if up else (z > 0))
                pl.when(at)(unit_copy(source, chip, d - 1, up).wait_recv)
                if d < nz - 1:
                    start(unit_copy(source, chip, d, up), onward)
            start(unit_mate(source), (source >= 0) & (source < rows))

    inputs = [
        pltpu.make_async_copy(pt_ref.at[part(h), :], gathered[h].at[c], in_sem.at[h])
        for h in range(PARTS)
    ]
    inputs.append(pltpu.make_async_copy(u_ref, unit_own, in_sem.at[PARTS]))
    inputs.append(pltpu.make_async_copy(pivot_hbm, pivot_ref, in_sem.at[PARTS + 1]))
    for copy in inputs:
        copy.start()

    def prepare(t):
        a_copy(t).wait()
        for s in range(slots):
            column = table_ref[2 * slots + s] * BLK
            high, low = halves(stage[t % 2][:, pl.ds(column, BLK)])
            a_high[pl.ds(t * tile_rows, tile_rows), s * BLK : (s + 1) * BLK] = high
            a_low[pl.ds(t * tile_rows, tile_rows), s * BLK : (s + 1) * BLK] = low
        if t + 2 < A_TILES:
            a_copy(t + 2).start()

    def z_copy(source, h, d, up):
        send, recv = (up_s, up_r) if up else (dn_s, dn_r)
        target = r + 2 if up else r - 2
        where = pt.at[source, part(h), :]
        return remote(where, where, send.at[d, h], recv.at[d, h], (target, c))

    def core_copy(source, h):
        where = pt.at[source, part(h), :]
        return remote(where, where, core_s.at[source // 2, h], core_r.at[source // 2, h], (mate, c))

    def own_part(h):
        for i in range(cols - 1):
            own_copy(h, i, plane[i]).wait_recv()
        inputs[h].wait()
        for s in range(slots):
            offset = table_ref[slots + s] * BLK
            value = gathered[h][table_ref[s], :, pl.ds(offset, BLK)]
            pt[r, part(h), s * BLK : (s + 1) * BLK] = value * table_ref[3 * slots + s].astype(jnp.float32)
        start(z_copy(r, h, 0, True), z < nz - 1)
        start(z_copy(r, h, 0, False), z > 0)
        start(core_copy(r, h))

    def tick(d, h):
        for up in (True, False):
            source = r - 2 * d if up else r + 2 * d
            there = (source >= 0) & (source < rows)
            onward = there & ((z < nz - 1) if up else (z > 0))
            pl.when(there)(lambda: z_copy(source, h, d - 1, up).wait_recv())
            if d < nz - 1:
                start(z_copy(source, h, d, up), onward)
            start(core_copy(source, h), there)

    def chip_at(j):
        near = jnp.where(z <= nz - 1 - z, z, nz - 1 - z)
        hop = (j + 1) // 2
        paired = z + hop if j % 2 else z - hop
        single = jnp.where(z <= nz - 1 - z, j, nz - 1 - j)
        return jnp.where(j <= 2 * near, paired, single)

    def pack(j):
        chip = chip_at(j)
        for h in range(PARTS):
            source = 2 * chip + 1 - p
            where = pt.at[source, part(h), :]
            remote(where, where, core_s.at[chip, h], core_r.at[chip, h], (mate, c)).wait_recv()
        for core in range(2):
            high, low = halves(pt[2 * chip + core])
            packed[core * kw : (core + 1) * kw, :] = high
            packed[(2 + core) * kw : (3 + core) * kw, :] = low

    def multiply(j, q, half):
        at = pl.ds(pl.multiple_of(q * rq + half * hq, 8), hq)
        both = dot(a_high[at, :], packed[...], NT)
        cross = dot(a_low[at, :], packed[: 2 * kw, :], NT)
        m_ref[j, at, :] = both[:, : 2 * kw] + (both[:, 2 * kw :] + cross)

    def tiles(q, half):
        return pl.ds(pl.multiple_of(q * rq + half * hq, 8), hq)

    first = ((xc, 0, xc, 0), (yc, 1, yc, 0), (dc, 0, xc, 1), (dc, 1, yc, 1))
    later = ((yc, 0), (xc, 1), (c, 0), (c, 1))

    def r1_copy(j, i):
        q, half, other, slot = first[i]
        return remote(
            m_ref.at[j, tiles(q, half), :],
            r1.at[j, half, slot],
            r1_s.at[j, half, slot],
            r1_r.at[j, half, slot],
            (r, other),
        )

    def r2_copy(j, half):
        return remote(
            r1.at[j, half, 1], r2.at[j, half], r2_s.at[j, half], r2_r.at[j, half],
            (r, xc if half else yc),
        )

    def product_tile(j, i):
        if i < 4:
            q, half, _, _ = first[i]
        else:
            q, half = later[i - 4]
        multiply(j, q, half)
        if i < 4:
            start(r1_copy(j, i))

    def reduce_first(j):
        for half in range(2):
            for i in range(4):
                if first[i][1] == half and first[i][3] == 1:
                    r1_copy(j, i).wait_recv()
            r1[j, half, 1] = r1[j, half, 1] + m_ref[j, tiles(xc if half else yc, half), :]
            start(r2_copy(j, half))

    def reduce_last(j):
        lanes = pl.ds(pl.multiple_of(chip_at(j) * 2 * kw, BLK), 2 * kw)
        for half in range(2):
            for i in range(4):
                if first[i][1] == half and first[i][3] == 0:
                    r1_copy(j, i).wait_recv()
            r2_copy(j, half).wait_recv()
            final[half * hq : (half + 1) * hq, lanes] = (
                m_ref[j, tiles(c, half), :] + r1[j, half, 0] + r2[j, half]
            )

    def listed_part(h):
        for target in range(rows):
            for k in range(quarter):
                at = 4 * slots + 3 * (target * quarter + k)
                offset = table_ref[at + 1] * BLK
                value = gathered[h][table_ref[at], :, pl.ds(offset, BLK)]
                ph_send[target, part(h), k * BLK : (k + 1) * BLK] = (
                    value * table_ref[at + 2].astype(jnp.float32)
                )

    def listed_send():
        for step in range(1, rows):
            target = (r + step) % rows
            start(
                remote(
                    ph_send.at[target], ph_recv.at[r], ph_s.at[step], ph_r.at[step], (target, c)
                )
            )
        ph_recv[r] = ph_send[r]

    def turn_unit():
        inputs[PARTS].wait()
        uf[r] = unit_own[...]
        for chip in range(nz):
            unit_mate(2 * chip + 1 - p).wait_recv()
        for chip in range(nz):
            both = jnp.concatenate([uf[2 * chip], uf[2 * chip + 1]], axis=0)
            high, low = halves(both.T)
            ut_high[:, chip * 2 * kw : (chip + 1) * 2 * kw] = high
            ut_low[:, chip * 2 * kw : (chip + 1) * 2 * kw] = low

    def normalise_listed():
        for step in range(1, rows):
            source = (r - step + rows) % rows
            remote(
                ph_send.at[source], ph_recv.at[source], ph_s.at[step], ph_r.at[step], (r, c)
            ).wait_recv()
        value = halves(ph_recv[...].reshape(width, rq))
        high, low = halves(dot3((ut_high[...], ut_low[...]), value, NN))
        nh_high[...] = high
        nh_low[...] = low

    def out_copy(i, other, source):
        return remote(
            cit.at[pl.ds(pl.multiple_of(other * wq, 8), wq), :],
            out_ref.at[:, pl.ds(pl.multiple_of(source * rq, BLK), rq)],
            out_s.at[i],
            out_r.at[i],
            (r, other),
        )

    def unit_product():
        cit[...] = -dot3((ut_high[...], ut_low[...]), halves(final[...]), NT)
        for i, other in enumerate(plane):
            start(out_copy(i, other, c))
        out_ref[:, pl.ds(pl.multiple_of(c * rq, BLK), rq)] = cit[
            pl.ds(pl.multiple_of(c * wq, 8), wq), :
        ]

    core_sum = remote(qp.at[1 - p], qc, qc_s, qc_r, (mate, c))

    def listed_product():
        ci = halves(cit[...])
        for chip in range(nz):
            at = slice(chip * 2 * kw, (chip + 1) * 2 * kw)
            value = dot3((nh_high[at, :], nh_low[at, :]), ci, NT)
            qp[0, chip] = value[:kw]
            qp[1, chip] = value[kw:]
        start(core_sum)

    def lanes_of(column):
        return pl.ds(pl.multiple_of(column * wq, BLK), wq)

    def plane_copy(i, other):
        return remote(qc.at[:, :, lanes_of(other)], qb.at[i], qb_s.at[i], qb_r.at[i], (r, other))

    def sum_cores():
        core_sum.wait_recv()
        qc[...] = qc[...] + qp[p]
        for i, other in enumerate(plane):
            start(plane_copy(i, other))

    def sum_plane():
        for i, other in enumerate(plane):
            plane_copy(i, other).wait_recv()
        qd[...] = qc[:, :, lanes_of(c)] + (qb[0] + (qb[1] + qb[2]))
        for step in range(1, nz):
            target = (z + step) % nz
            start(
                remote(
                    qd.at[target], qz.at[step], qz_s.at[step], qz_r.at[step], (2 * target + p, c)
                )
            )

    def sum_line():
        for step in range(1, nz):
            remote(qd.at[step], qz.at[step], qz_s.at[step], qz_r.at[step], (r, c)).wait_recv()
        total = qd[z]
        for step in range(1, nz):
            total = total + qz[step]
        inputs[PARTS + 1].wait()
        diag_ref[...] = pivot_ref[...] - total

    def finish():
        for i, other in enumerate(plane):
            out_copy(i, other, other).wait_recv()
        for copy, when in sent:
            if when is None:
                copy.wait_send()
            else:
                pl.when(when)(copy.wait_send)

    prepare(0)
    prepare(1)
    prepare(2)
    prepare(3)
    own_send(1)
    unit_tick(1)
    prepare(4)
    own_part(0)
    own_send(2)
    unit_tick(2)
    prepare(5)
    own_part(1)
    own_send(3)
    tick(1, 0)
    own_part(2)
    tick(1, 1)
    own_part(3)
    tick(2, 0)
    unit_tick(3)
    tick(1, 2)

    between = {
        (0, 1): (2, 1), (0, 3): (1, 3), (0, 7): (2, 2), (1, 7): (2, 3), (2, 1): (3, 0),
        (2, 3): (3, 1), (2, 5): (3, 2), (2, 7): (3, 3),
    }
    for j in range(nz):
        pack(j)
        if j == nz - 1:
            listed_send()
        for i in range(8):
            product_tile(j, i)
            if (j, i) in between:
                tick(*between[j, i])
            if j == 0 and i == 4:
                for h in range(PARTS):
                    listed_part(h)
            if j == 1 and i == 4:
                turn_unit()
            if j >= 1 and i == 4:
                reduce_first(j - 1)
            if j >= 2 and i == 6:
                reduce_last(j - 2)
    reduce_first(nz - 1)
    reduce_last(nz - 2)
    reduce_last(nz - 1)
    unit_product()
    normalise_listed()
    listed_product()
    sum_cores()
    sum_plane()
    sum_line()
    finish()


def fused(rows, cols, ancestor_inverse, panel, unit_inverse, pivot_inverse, panel_blocks):
    rows_here, cols_here = ancestor_inverse.shape
    stored, kw = panel.shape
    width = unit_inverse.shape[1]
    row_blocks, range_blocks = rows_here // BLK, cols_here // BLK
    table = tables(panel_blocks, cols, range_blocks, row_blocks, rows)
    slots = range_blocks // 2
    chosen = slots * BLK
    nz = rows // 2
    rq, wq = rows_here // cols, width // cols
    f32, bf16 = jnp.float32, jnp.bfloat16
    dma = pltpu.SemaphoreType.DMA
    vmem = pl.BlockSpec(memory_space=pltpu.VMEM)
    smem = pl.BlockSpec(memory_space=pltpu.SMEM)
    scratch = (
        [pltpu.VMEM((cols, kw // PARTS, stored), f32)] * PARTS
        + [pltpu.VMEM((rows_here // A_TILES, cols_here), f32)] * 2
        + [
            pltpu.VMEM((rows, kw, chosen), f32),
            pltpu.VMEM((4 * kw, chosen), bf16),
            pltpu.VMEM((rows_here, chosen), bf16),
            pltpu.VMEM((rows_here, chosen), bf16),
            pltpu.VMEM((nz, rows_here, 2 * kw), f32),
            pltpu.VMEM((nz, 2, 2, rq // 2, 2 * kw), f32),
            pltpu.VMEM((nz, 2, rq // 2, 2 * kw), f32),
            pltpu.VMEM((rq, width), f32),
            pltpu.VMEM((rows, kw, width), f32),
            pltpu.VMEM((width, width), bf16),
            pltpu.VMEM((width, width), bf16),
            pltpu.VMEM((rows, kw, rq), f32),
            pltpu.VMEM((rows, kw, rq), f32),
            pltpu.VMEM((width, rq), bf16),
            pltpu.VMEM((width, rq), bf16),
            pltpu.VMEM((width, rq), f32),
            pltpu.VMEM((2, nz, kw, width), f32),
            pltpu.VMEM((nz, kw, width), f32),
            pltpu.VMEM((cols - 1, nz, kw, wq), f32),
            pltpu.VMEM((nz, kw, wq), f32),
            pltpu.VMEM((nz, kw, wq), f32),
            pltpu.VMEM(unit_inverse.shape, f32),
            pltpu.VMEM(pivot_inverse.shape, f32),
            dma((PARTS + 2,)),
            dma((2,)),
            dma((PARTS, cols - 1)),
            dma((PARTS, cols - 1)),
            dma((nz, PARTS)),
            dma((nz, PARTS)),
            dma((nz, PARTS)),
            dma((nz, PARTS)),
            dma((nz, PARTS)),
            dma((nz, PARTS)),
            dma((nz,)),
            dma((nz,)),
            dma((nz,)),
            dma((nz,)),
            dma((nz,)),
            dma((nz,)),
            dma((rows,)),
            dma((rows,)),
            dma((nz, 2, 2)),
            dma((nz, 2, 2)),
            dma((nz, 2)),
            dma((nz, 2)),
            dma((cols - 1,)),
            dma((cols - 1,)),
            dma,
            dma,
            dma((cols - 1,)),
            dma((cols - 1,)),
            dma((nz,)),
            dma((nz,)),
        ]
    )
    return pl.pallas_call(
        functools.partial(fused_kernel, rows, cols),
        out_shape=(
            jax.ShapeDtypeStruct((wq, rows_here), f32),
            jax.ShapeDtypeStruct(pivot_inverse.shape, f32),
        ),
        in_specs=[smem] + [pl.BlockSpec(memory_space=pltpu.HBM)] * 4,
        out_specs=(vmem, vmem),
        scratch_shapes=scratch,
        compiler_params=pltpu.CompilerParams(
            collective_id=0, has_side_effects=True, vmem_limit_bytes=50 << 20
        ),
    )(table, panel.T, unit_inverse, pivot_inverse, ancestor_inverse)


def fits(mesh, ancestor_inverse, panel, unit_inverse):
    rows, cols = mesh.shape["row"], mesh.shape["col"]
    rows_here = ancestor_inverse.shape[0] // rows
    width = unit_inverse.shape[1]
    return (
        cols == 4
        and rows % 2 == 0
        and rows_here % (cols * BLK) == 0
        and rows_here % (16 * A_TILES) == 0
        and width == BLK * (rows // 2)
        and panel.shape[0] % (cols * BLK) == 0
        and ancestor_inverse.shape[1] % (2 * cols * BLK) == 0
    )


def solution(mesh):
    rows, cols = mesh.shape["row"], mesh.shape["col"]

    def whole(ancestor_inverse, panel, unit_inverse, pivot_inverse, panel_blocks):
        body = on_device
        if fits(mesh, ancestor_inverse, panel, unit_inverse):
            body = functools.partial(fused, rows, cols)
        return jax.shard_map(
            body,
            mesh=mesh,
            in_specs=(P("row", "col"), P("col", "row"), P("row", None), P("row", "col"), P()),
            out_specs=(P("col", "row"), P("row", "col")),
            check_vma=False,
        )(ancestor_inverse, panel, unit_inverse, pivot_inverse, panel_blocks)

    return whole
```
